256 devices in a mesh: rows: 8 (over y, core), cols: 16 (over z_hi, x), hub: 2 (over z_lo).
Axes of the slice: x: 4, y: 4, z: 8 (z_hi: 4, z_lo: 2; z = z_hi * 2 + z_lo), core: 2. Of those that a mesh axis runs over, the one named last changes fastest.
Arguments:
- light_bits: int32 [384, 12288], P('rows', 'cols'), may hold values from -2147483648 to 2147483647, as said below
- hub_bits: int32 [8, 12288], P('hub', 'cols'), may hold values from -2147483648 to 2147483647, as said below
- hub_ids: int32 [256], replicated, may hold values from 0 to 12287, as said below
Outputs:
- clustering: float32 [12288], P(('rows', 'cols'))
The draws below stay inside these ranges and needn't reach their ends.
Inputs may be any that keep to these rules, and one draw needn't show every extreme that they name: Every word holds 32 bits; the matrix of light_bits is symmetric with a zero diagonal. `hub_bits`: every word holds 32 bits. `hub_ids`: 256 distinct vertex numbers.
All inputs are finite; a program needn't handle non-finite values.
Results may differ from the reference program's by a relative error of at most 0.0003.
Values sent between devices are 32-bit elements; how exact they have to be, the bound alone decides.
A program may use at most 128 MiB of HBM per device.

```python
import jax
import jax.numpy as jnp
from jax import lax

VERTICES = 12288
HUBS = 256


def vertex_weights(key):
    vertex_rank = jax.random.permutation(jax.random.fold_in(key, 7), VERTICES).astype(jnp.int32)
    weight = 4 + 128 // (1 + vertex_rank // 32)
    return (vertex_rank, weight)


def pack_bits(linked):
    powers = jnp.left_shift(jnp.int32(1), jnp.arange(32, dtype=jnp.int32))
    grouped = linked.astype(jnp.int32).reshape(linked.shape[0] // 32, 32, linked.shape[1])
    return jnp.sum(grouped * powers[None, :, None], axis=1).astype(jnp.int32)


def draw_light_bits(key, part):
    vertex_rank, weight = vertex_weights(key)
    samples = jax.random.randint(jax.random.fold_in(key, 11), (VERTICES, VERTICES), 0, 8192, dtype=jnp.int32)
    linked = samples < weight[:, None] * weight[None, :]
    vertex_ids = jnp.arange(VERTICES, dtype=jnp.int32)
    one_side = jnp.logical_and(linked, vertex_ids[None, :] > vertex_ids[:, None])
    symmetric = jnp.logical_or(one_side, one_side.T)
    return pack_bits(symmetric)


def draw_hub_bits(key, part):
    vertex_rank, weight = vertex_weights(key)
    samples = jax.random.randint(jax.random.fold_in(key, 13), (HUBS, VERTICES), 0, 1024, dtype=jnp.int32)
    linked = samples < 48 + weight[None, :]
    return pack_bits(linked)


def draw_hub_ids(key, part):
    vertex_rank, weight = vertex_weights(key)
    by_rank = jnp.argsort(vertex_rank)
    return by_rank[:HUBS].astype(jnp.int32)


def setup_inputs(seed: int = 0) -> dict:
    streams_of = jax.random.split(jax.random.key(seed), 4)
    return {
        "light_bits": draw_light_bits(jax.random.fold_in(streams_of[3], 71), 0),
        "hub_bits": draw_hub_bits(jax.random.fold_in(streams_of[3], 71), 0),
        "hub_ids": draw_hub_ids(jax.random.fold_in(streams_of[3], 71), 0),
    }


def unpack(packed):
    shifts = jnp.arange(32, dtype=jnp.int32)
    bit_grid = jnp.bitwise_and(jnp.right_shift(packed[:, None, :], shifts[None, :, None]), 1)
    return bit_grid.reshape(packed.shape[0] * 32, packed.shape[1]).astype(jnp.float32)


def reference(light_bits, hub_bits, hub_ids):
    total = light_bits.shape[1]
    vertex_ids = jnp.arange(total, dtype=jnp.int32)
    is_hub = jnp.any(vertex_ids[:, None] == hub_ids[None, :], axis=1)
    light = jnp.where(is_hub, 0.0, 1.0).astype(jnp.float32)
    adjacency = unpack(light_bits) * light[:, None] * light[None, :]
    two_paths = jnp.dot(adjacency, adjacency, precision=lax.Precision.HIGHEST, preferred_element_type=jnp.float32)
    light_tri = 0.5 * jnp.sum(adjacency * two_paths, axis=1)
    hub_rows = unpack(hub_bits) * light[None, :]
    reach_hub = jnp.dot(hub_rows, adjacency, precision=lax.Precision.HIGHEST, preferred_element_type=jnp.float32)
    intersect = hub_rows * reach_hub
    hub_tri = 0.5 * jnp.sum(intersect, axis=1)
    hub_deg = jnp.sum(hub_rows, axis=1)
    owners = (vertex_ids[:, None] == hub_ids[None, :]).astype(jnp.float32)
    triangles = light_tri + jnp.sum(intersect, axis=0) + jnp.sum(owners * hub_tri[None, :], axis=1)
    degrees = jnp.sum(adjacency, axis=1) + jnp.sum(hub_rows, axis=0) + jnp.sum(owners * hub_deg[None, :], axis=1)
    return triangles / (1.0 + degrees)
```

```python
import functools

import jax
import jax.numpy as jnp
from jax import lax
from jax.experimental import pallas as pl
from jax.experimental.pallas import tpu as pltpu
from jax.sharding import PartitionSpec as P

MESH = pl.DeviceIdType.MESH
F32 = jnp.float32
F8 = jnp.float8_e4m3fn

THIRD = [
    0, 0, 47, 11, 19, 60, 25, 61, 42, 60, 37, 30, 41, 62, 26, 47,
    52, 16, 9, 9, 6, 34, 46, 19, 20, 46, 59, 37, 52, 19, 60, 48,
    1, 53, 11, 47, 18, 18, 29, 57, 53, 33, 13, 59, 6, 39, 41, 62,
    34, 6, 56, 12, 52, 16, 27, 27, 22, 4, 39, 40, 56, 52, 55, 13,
    14, 24, 25, 56, 56, 19, 43, 15, 36, 36, 57, 29, 50, 57, 15, 43,
    57, 2, 14, 2, 2, 38, 49, 26, 38, 2, 45, 45, 22, 4, 3, 62,
    19, 32, 56, 41, 43, 10, 13, 19, 5, 35, 25, 47, 54, 54, 47, 3,
    6, 12, 11, 21, 20, 24, 26, 32, 32, 22, 44, 10, 10, 38, 63, 63,
]


def destinations():
    rows, cols = [0] * 128, [0] * 128
    for i in range(8):
        for j in range(8):
            for h in range(2):
                for s in range(2):
                    k = THIRD[(i * 8 + j) * 2 + h] >> (3 * s) & 7
                    if i != j and k != j:
                        rows[(i * 8 + k) * 2 + h] |= 1 << (2 * j + s)
                    if i != j and k != i:
                        cols[(k * 8 + j) * 2 + h] |= 1 << (2 * i + s)
    return rows, cols


def lookup(tables, index, bits):
    tables = [list(t) for t in tables]
    for b in range(bits):
        bit = lax.rem(lax.div(index, 2**b), 2)
        for n, t in enumerate(tables):
            pairs = []
            for low, high in zip(t[0::2], t[1::2]):
                if isinstance(low, int) and isinstance(high, int) and low == high:
                    pairs.append(low)
                else:
                    pairs.append(low + bit * (high - low))
            tables[n] = pairs
    return [t[0] for t in tables]


def bit_of(mask, n):
    return lax.rem(lax.div(mask, lax.shift_left(jnp.int32(1), n)), 2) == 1


def rows_of_bits(words, first, count):
    shift = lax.broadcasted_iota(jnp.int32, (32, words.shape[1]), 0)
    spread = [jnp.broadcast_to(words[w : w + 1, :], shift.shape) for w in range(first, first + count)]
    return [jnp.bitwise_and(jnp.right_shift(x, shift), 1) for x in spread]


def unpack_into(dst, src, words, lane=0):
    width = src.shape[1]

    def step(g, carry):
        block = src[pl.ds(pl.multiple_of(g * 8, 8), 8), :]
        for n, bits in enumerate(rows_of_bits(block, 0, 8)):
            at = pl.multiple_of(g * 256 + n * 32, 32)
            dst[pl.ds(at, 32), lane : lane + width] = bits.astype(F32).astype(dst.dtype)
        return carry

    lax.fori_loop(0, words // 8, step, 0)


def kernel(
    lb, hb, ids_s, ids_v, out,
    m1, m2, m3, mm1, hubw, hub_i, a8, b8, o8, r8,
    acc_r, acc_c, col, col_in, hpart, h_in, segs, inbox,
    local_sem, send_sem, recv_sem, hub_send, hub_recv, ha_send, ha_recv, cs_sem, cr_sem, fs_sem, fr_sem,
):
    I = lax.axis_index("rows")
    c = lax.axis_index("cols")
    h = lax.axis_index("hub")
    J = lax.div(c, 2)
    s = lax.rem(c, 2)
    o = 1 - s
    W = m1.shape[1]
    C = m1.shape[2]
    B = 2 * C
    diag = I == J

    load_l = pltpu.make_async_copy(lb, m1.at[s], local_sem.at[0])
    load_h = pltpu.make_async_copy(hb, hubw, local_sem.at[1])
    load_l.start()
    load_h.start()

    barrier = pltpu.get_barrier_semaphore()

    def signal(dev):
        pl.semaphore_signal(barrier, inc=1, device_id=dev, device_id_type=MESH)

    def greet_plane(n, carry):
        @pl.when(n != c * 2 + h)
        def _():
            signal((I, lax.div(n, 2), lax.rem(n, 2)))

        return carry

    def greet_column(n, carry):
        @pl.when(lax.div(n, 2) != I)
        def _():
            signal((lax.div(n, 2), 2 * J + lax.rem(n, 2), h))

        return carry

    lax.fori_loop(0, 32, greet_plane, 0)
    lax.fori_loop(0, 16, greet_column, 0)

    to_rows, to_cols, thirds = lookup([ROWS_TO, COLS_TO, THIRD], (I * 8 + J) * 2 + h, 7)
    K = lax.rem(lax.div(thirds, 1 + 7 * s), 8)

    lane_w = lax.broadcasted_iota(jnp.int32, (8, 128), 1)
    sub_w = lax.broadcasted_iota(jnp.int32, (8, 128), 0)
    word_id = jnp.where(sub_w == 0, I * W, K * W) + lane_w
    word_id = jnp.where(lane_w < W, word_id, -1)
    col_id = J * B + lax.broadcasted_iota(jnp.int32, (16, 128), 0) * 128 + lax.broadcasted_iota(jnp.int32, (16, 128), 1)

    def mark(g, carry):
        words, flags = carry
        for n in range(16):
            v = ids_s[g * 16 + n]
            words = words | jnp.where(
                word_id == jnp.right_shift(v, 5), jnp.left_shift(jnp.int32(1), jnp.bitwise_and(v, 31)), 0
            )
            flags = flags | (col_id == v).astype(jnp.int32)
        return words, flags

    words, flags = lax.fori_loop(
        0, 16, mark, (jnp.zeros((8, 128), jnp.int32), jnp.zeros((16, 128), jnp.int32))
    )
    keep_words = jnp.bitwise_not(words)
    keep_i = jnp.broadcast_to(keep_words[0:1, :], (128, 128)).T[:W]
    keep_k = jnp.broadcast_to(keep_words[1:2, :], (128, 128)).T[:W]
    keep_col = flags - 1

    load_l.wait()
    load_h.wait()
    pl.semaphore_wait(barrier, 45)

    own = m1.at[s]

    def to_row(n):
        return pltpu.make_async_remote_copy(
            own, m2.at[s], send_sem.at[n], recv_sem.at[2 + s], device_id=(I, n, h), device_id_type=MESH
        )

    def to_col(n):
        return pltpu.make_async_remote_copy(
            own,
            m3.at[s],
            send_sem.at[16 + n],
            recv_sem.at[4 + s],
            device_id=(lax.div(n, 2), 2 * J + lax.rem(n, 2), h),
            device_id_type=MESH,
        )

    def to_twin():
        return pltpu.make_async_remote_copy(
            own, m1.at[s], send_sem.at[32], recv_sem.at[s], device_id=(I, c + 1 - 2 * s, h), device_id_type=MESH
        )

    def to_hub(n):
        return pltpu.make_async_remote_copy(
            hubw, hub_i.at[s], hub_send.at[n], hub_recv.at[s], device_id=(I, n, h), device_id_type=MESH
        )

    def each_hub(act):
        @pl.when(diag)
        def _():
            def step(n, carry):
                @pl.when(n != c)
                def _():
                    act(to_hub(n))

                return carry

            lax.fori_loop(0, 16, step, 0)

    def each_block(act):
        def step(n, carry):
            @pl.when(bit_of(to_cols, n))
            def _():
                act(to_col(n))

            @pl.when(bit_of(to_rows, n))
            def _():
                act(to_row(n))

            return carry

        lax.fori_loop(0, 16, step, 0)
        act(to_twin())

    each_hub(lambda d: d.start())
    each_block(lambda d: d.start())

    def mask_half(half):
        for t in range(C // 128):
            at = slice(t * 128, t * 128 + 128)
            lanes = keep_cols_of(half, t)
            mm1[half, :, at] = m1[half, :, at] & keep_i & lanes

    def keep_cols_of(half, t):
        if isinstance(half, int):
            return keep_col[half * (C // 128) + t : half * (C // 128) + t + 1, :]
        return jnp.where(half == 0, keep_col[t : t + 1, :], keep_col[C // 128 + t : C // 128 + t + 1, :])

    mask_half(s)
    unpack_into(o8, mm1.at[s], W)

    @pl.when(diag)
    def _():
        hub_i[s] = hubw[...]

    def hub_half(half):
        pltpu.make_async_copy(hubw, hub_i.at[half], hub_recv.at[half]).wait()

    @pl.when(jnp.logical_not(diag))
    def _():
        hub_half(s)

    hub_half(o)
    G = hubw.shape[0]
    for half in range(2):
        for n, bits in enumerate(rows_of_bits(hub_i[half], 0, G)):
            r8[n * 32 : n * 32 + 32, half * C : half * C + C] = bits.astype(F32).astype(F8)
    reach = jnp.dot(r8[...], o8[...], preferred_element_type=F32)
    edge = hubw[...]
    lanes_c = jnp.concatenate([keep_cols_of(s, t) for t in range(C // 128)], axis=1)
    edge = edge & lanes_c
    hub_bits = jnp.concatenate(rows_of_bits(edge, 0, G), axis=0)
    meet = jnp.where(hub_bits != 0, reach, 0.0)
    hub_flag = hub_bits.astype(F32)

    def across(x):
        t = x[:, 0:128]
        for n in range(1, x.shape[1] // 128):
            t = t + x[:, n * 128 : n * 128 + 128]
        return jnp.sum(t.T, axis=0, keepdims=True)

    hub_tri = 0.5 * across(meet)
    hub_deg = across(hub_flag)
    hpart[...] = hub_tri

    def to_column(n):
        return pltpu.make_async_remote_copy(
            hpart, h_in.at[I], ha_send.at[n], ha_recv.at[I], device_id=(n, c, h), device_id_type=MESH
        )

    def others(act):
        def step(n, carry):
            @pl.when(n != I)
            def _():
                act(n)

            return carry

        lax.fori_loop(0, 8, step, 0)

    others(lambda n: to_column(n).start())

    light_deg = jnp.sum(lax.population_count(mm1[s]).astype(F32), axis=0, keepdims=True) * 0.5
    edge_deg = jnp.sum(lax.population_count(edge).astype(F32), axis=0, keepdims=True)
    col_deg = light_deg + jnp.where(diag, 1.0, 0.0) * edge_deg
    col_tri = jnp.sum(meet, axis=0, keepdims=True)
    zero = jnp.zeros((1, C), F32)
    for half in range(2):
        here = s == half
        col[0:1, half * C : half * C + C] = jnp.where(here, col_tri, zero)
        col[1:2, half * C : half * C + C] = jnp.where(here, col_deg, zero)

    def recv(ref, sem):
        pltpu.make_async_copy(own, ref, sem).wait()

    recv(m1.at[o], recv_sem.at[o])
    mask_half(o)

    @pl.when(K != J)
    def _():
        recv(m2.at[0], recv_sem.at[2])
        recv(m2.at[1], recv_sem.at[3])

    @pl.when(K == J)
    def _():
        m2[...] = m1[...]

    unpack_into(a8, m2.at[0], W, 0)
    unpack_into(a8, m2.at[1], W, C)

    @pl.when(K != I)
    def _():
        recv(m3.at[0], recv_sem.at[4])
        recv(m3.at[1], recv_sem.at[5])

    @pl.when(K == I)
    def _():
        m3[...] = m1[...]

    for half in range(2):
        for t in range(C // 128):
            at = slice(t * 128, t * 128 + 128)
            m3[half, :, at] = m3[half, :, at] & keep_k
    unpack_into(b8, m3.at[0], W, 0)
    unpack_into(b8, m3.at[1], W, C)

    acc_r[...] = jnp.zeros_like(acc_r)
    MC, NC = 512, 256
    shift = lax.broadcasted_iota(jnp.int32, (32, NC), 0)

    for half in range(2):

        def chunk(n, carry, half=half):
            at = pl.multiple_of(n * NC, NC)
            sums = jnp.zeros((8, NC), F32)
            for m in range(B // MC):
                paths = jnp.dot(
                    a8[m * MC : m * MC + MC, :],
                    b8[:, pl.ds(pl.multiple_of(half * C + n * NC, NC), NC)],
                    preferred_element_type=F32,
                )
                for w in range(MC // 32):
                    word = m * (MC // 32) + w
                    x = jnp.broadcast_to(mm1[half, word : word + 1, pl.ds(at, NC)], (32, NC))
                    bits = jnp.bitwise_and(jnp.right_shift(x, shift), 1)
                    t = jnp.where(bits != 0, paths[w * 32 : w * 32 + 32], 0.0)
                    sums = sums + jnp.sum(t.reshape(4, 8, NC), axis=0)
                    acc_r[word * 32 : word * 32 + 32, :] += t[:, :128] + t[:, 128:]
            acc_c[:, pl.ds(pl.multiple_of(half * C + n * NC, NC), NC)] = sums
            return carry

        lax.fori_loop(0, C // NC, chunk, 0)

    row_w = jnp.where(diag, 0.125, jnp.where(K == I, 1.0, 0.5))
    col_w = jnp.where(diag, 0.0, jnp.where(K == J, 1.0, 0.5))
    col[0:1, :] += col_w * jnp.sum(acc_c[...], axis=0, keepdims=True)

    def to_diag():
        return pltpu.make_async_remote_copy(
            col, col_in.at[I], cs_sem, cr_sem.at[I], device_id=(J, c, h), device_id_type=MESH
        )

    @pl.when(jnp.logical_not(diag))
    def _():
        to_diag().start()

    def wait_hub(n):
        pltpu.make_async_copy(hpart, h_in.at[n], ha_recv.at[n]).wait()

    h_in[I] = hpart[...]
    others(wait_hub)
    hub_all = h_in[0]
    for n in range(1, 8):
        hub_all = hub_all + h_in[n]
    V = out.shape[1]
    pad = jnp.zeros((1, 128 - V), F32)
    for n in range(B // V):
        part = jnp.sum(acc_r[n * V : n * V + V, :].T, axis=0, keepdims=True) * row_w
        segs[n, 0:1, :] = jnp.concatenate([part, pad], axis=1)
        segs[n, 1:2, :] = jnp.zeros((1, 128), F32)
        segs[n, 2:3, :] = hub_all
        segs[n, 3:4, :] = hub_deg

    @pl.when(diag)
    def _():
        def wait_col(n):
            pltpu.make_async_copy(col, col_in.at[n], cr_sem.at[n]).wait()

        others(wait_col)
        col_in[I] = col[...]
        whole = col_in[0]
        for n in range(1, 8):
            whole = whole + col_in[n]
        for n in range(B // V):
            segs[n, 0:2, 0:V] += whole[:, n * V : n * V + V]

    me = c * 2 + h

    def to_plane(n):
        return pltpu.make_async_remote_copy(
            segs.at[lax.div(n, 2)],
            inbox.at[me],
            fs_sem.at[n],
            fr_sem.at[me],
            device_id=(I, lax.div(n, 2), lax.rem(n, 2)),
            device_id_type=MESH,
        )

    def plane(act):
        def step(n, carry):
            @pl.when(n != me)
            def _():
                act(n)

            return carry

        lax.fori_loop(0, 32, step, 0)

    plane(lambda n: to_plane(n).start())
    inbox[me] = segs[c]

    vertex = I * B + c * V + lax.broadcasted_iota(jnp.int32, (V, 128), 0)
    is_hub = [vertex == ids_v[g : g + 1, :] for g in range(2)]

    plane(lambda n: pltpu.make_async_copy(segs.at[0], inbox.at[n], fr_sem.at[n]).wait())
    even = inbox[0]
    odd = inbox[1]
    for n in range(1, 16):
        even = even + inbox[2 * n]
        odd = odd + inbox[2 * n + 1]
    both = even + odd

    def at_hubs(r):
        rows = [jnp.broadcast_to(x[r : r + 1, :], (V, 128)) for x in (even, odd)]
        hit = jnp.where(is_hub[0], rows[0], 0.0) + jnp.where(is_hub[1], rows[1], 0.0)
        return jnp.sum(hit.T, axis=0, keepdims=True)

    tri = both[0:1, :V] + at_hubs(2)
    deg = both[1:2, :V] + at_hubs(3)
    out[...] = tri / (1.0 + deg)

    each_hub(lambda d: d.wait_send())
    each_block(lambda d: d.wait_send())
    others(lambda n: to_column(n).wait_send())

    @pl.when(jnp.logical_not(diag))
    def _():
        to_diag().wait_send()

    plane(lambda n: to_plane(n).wait_send())


ROWS_TO, COLS_TO = destinations()


def body(light_bits, hub_bits, hub_ids):
    W, C = light_bits.shape
    G = hub_bits.shape[0]
    B = 2 * C
    V = B // 16
    vmem = pl.BlockSpec(memory_space=pltpu.VMEM)
    out = pl.pallas_call(
        kernel,
        out_shape=jax.ShapeDtypeStruct((1, V), F32),
        in_specs=[
            pl.BlockSpec(memory_space=pl.ANY),
            pl.BlockSpec(memory_space=pl.ANY),
            pl.BlockSpec(memory_space=pltpu.SMEM),
            vmem,
        ],
        out_specs=vmem,
        scratch_shapes=[
            pltpu.VMEM((2, W, C), jnp.int32),
            pltpu.VMEM((2, W, C), jnp.int32),
            pltpu.VMEM((2, W, C), jnp.int32),
            pltpu.VMEM((2, W, C), jnp.int32),
            pltpu.VMEM((G, C), jnp.int32),
            pltpu.VMEM((2, G, C), jnp.int32),
            pltpu.VMEM((B, B), F8),
            pltpu.VMEM((B, B), F8),
            pltpu.VMEM((B, C), F8),
            pltpu.VMEM((32 * G, B), F8),
            pltpu.VMEM((B, 128), F32),
            pltpu.VMEM((8, B), F32),
            pltpu.VMEM((2, B), F32),
            pltpu.VMEM((8, 2, B), F32),
            pltpu.VMEM((1, 128), F32),
            pltpu.VMEM((8, 1, 128), F32),
            pltpu.VMEM((16, 4, 128), F32),
            pltpu.VMEM((32, 4, 128), F32),
            pltpu.SemaphoreType.DMA((2,)),
            pltpu.SemaphoreType.DMA((33,)),
            pltpu.SemaphoreType.DMA((6,)),
            pltpu.SemaphoreType.DMA((16,)),
            pltpu.SemaphoreType.DMA((2,)),
            pltpu.SemaphoreType.DMA((8,)),
            pltpu.SemaphoreType.DMA((8,)),
            pltpu.SemaphoreType.DMA,
            pltpu.SemaphoreType.DMA((8,)),
            pltpu.SemaphoreType.DMA((32,)),
            pltpu.SemaphoreType.DMA((32,)),
        ],
        compiler_params=pltpu.CompilerParams(
            collective_id=0, has_side_effects=True, vmem_limit_bytes=48 * 2**20
        ),
    )(light_bits, hub_bits, hub_ids, hub_ids.reshape(2, 128))
    return out.reshape(V)


def solution(mesh):
    placed = (P("rows", "cols"), P("hub", "cols"), P())
    return jax.shard_map(body, mesh=mesh, in_specs=placed, out_specs=P(("rows", "cols")), check_vma=False)
```

```python
import functools

import jax
import jax.numpy as jnp
from jax import lax
from jax.experimental import pallas as pl
from jax.experimental.pallas import tpu as pltpu
from jax.sharding import PartitionSpec as P

MESH = pl.DeviceIdType.MESH
F32 = jnp.float32
F8 = jnp.float8_e4m3fn

THIRD = [
    0, 0, 47, 11, 19, 60, 25, 61, 42, 60, 37, 30, 41, 62, 26, 47,
    52, 16, 9, 9, 6, 34, 46, 19, 20, 46, 59, 37, 52, 19, 60, 48,
    1, 53, 11, 47, 18, 18, 29, 57, 53, 33, 13, 59, 6, 39, 41, 62,
    34, 6, 56, 12, 52, 16, 27, 27, 22, 4, 39, 40, 56, 52, 55, 13,
    14, 24, 25, 56, 56, 19, 43, 15, 36, 36, 57, 29, 50, 57, 15, 43,
    57, 2, 14, 2, 2, 38, 49, 26, 38, 2, 45, 45, 22, 4, 3, 62,
    19, 32, 56, 41, 43, 10, 13, 19, 5, 35, 25, 47, 54, 54, 47, 3,
    6, 12, 11, 21, 20, 24, 26, 32, 32, 22, 44, 10, 10, 38, 63, 63,
]


def destinations():
    rows, cols = [0] * 128, [0] * 128
    for i in range(8):
        for j in range(8):
            for h in range(2):
                for s in range(2):
                    k = THIRD[(i * 8 + j) * 2 + h] >> (3 * s) & 7
                    if i != j and k != j:
                        rows[(i * 8 + k) * 2 + h] |= 1 << (2 * j + s)
                    if i != j and k != i:
                        cols[(k * 8 + j) * 2 + h] |= 1 << (2 * i + s)
    return rows, cols


def lookup(tables, index, bits):
    tables = [list(t) for t in tables]
    for b in range(bits):
        odd = lax.rem(lax.div(index, 2**b), 2) == 1
        tables = [
            [x if isinstance(x, int) and x is y else jnp.where(odd, y, x) for x, y in zip(t[0::2], t[1::2])]
            for t in tables
        ]
    return [t[0] for t in tables]


def bit_of(mask, n):
    return lax.rem(lax.div(mask, 2**n), 2) == 1


def rows_of_bits(words, first, count):
    shift = lax.broadcasted_iota(jnp.int32, (32, words.shape[1]), 0)
    spread = [jnp.broadcast_to(words[w : w + 1, :], shift.shape) for w in range(first, first + count)]
    return [jnp.bitwise_and(jnp.right_shift(x, shift), 1) for x in spread]


def unpack_into(dst, src, words, lane=0):
    width = src.shape[1]

    def step(g, carry):
        block = src[pl.ds(pl.multiple_of(g * 8, 8), 8), :]
        for n, bits in enumerate(rows_of_bits(block, 0, 8)):
            at = pl.multiple_of(g * 256 + n * 32, 32)
            dst[pl.ds(at, 32), lane : lane + width] = bits.astype(F32).astype(dst.dtype)
        return carry

    lax.fori_loop(0, words // 8, step, 0)


def kernel(
    lb, hb, ids, out,
    ids_s, ids_v, m1, m2, m3, mm1, hubw, hub_i, a8, b8, o8, r8,
    acc_r, acc_c, col, hpart, h_in, rmsg, cmsg, r_in, c_in,
    local_sem, send_sem, recv_sem, hub_send, hub_recv, ha_send, ha_recv, rs_sem, rr_sem, cs_sem, cr_sem,
):
    I = lax.axis_index("rows")
    c = lax.axis_index("cols")
    h = lax.axis_index("hub")
    J = lax.div(c, 2)
    s = lax.rem(c, 2)
    o = 1 - s
    W = m1.shape[1]
    C = m1.shape[2]
    B = 2 * C
    V = out.shape[1]
    diag = I == J
    off = jnp.logical_not(diag)

    loads = [
        pltpu.make_async_copy(lb, m1.at[s], local_sem.at[0]),
        pltpu.make_async_copy(hb, hubw, local_sem.at[1]),
        pltpu.make_async_copy(ids, ids_s, local_sem.at[2]),
        pltpu.make_async_copy(ids, ids_v, local_sem.at[3]),
    ]
    for load in loads:
        load.start()

    barrier = pltpu.get_barrier_semaphore()

    def signal(dev):
        pl.semaphore_signal(barrier, inc=1, device_id=dev, device_id_type=MESH)

    me = c * 2 + h
    for n in range(1, 32):
        peer = lax.rem(me + n, 32)
        signal((I, lax.div(peer, 2), lax.rem(peer, 2)))
    for n in range(1, 8):
        for half in range(2):
            signal((lax.rem(I + n, 8), 2 * J + half, h))

    to_rows, to_cols, thirds = lookup([ROWS_TO, COLS_TO, THIRD], (I * 8 + J) * 2 + h, 7)
    K = lax.rem(jnp.where(s == 1, lax.div(thirds, 8), thirds), 8)
    loads[0].wait()
    loads[1].wait()
    pl.semaphore_wait(barrier, 45)

    own = m1.at[s]

    def to_row(n):
        return pltpu.make_async_remote_copy(
            own, m2.at[s], send_sem.at[n], recv_sem.at[2 + s], device_id=(I, n, h), device_id_type=MESH
        )

    def to_col(n):
        return pltpu.make_async_remote_copy(
            own,
            m3.at[s],
            send_sem.at[16 + n],
            recv_sem.at[4 + s],
            device_id=(n // 2, 2 * J + n % 2, h),
            device_id_type=MESH,
        )

    def to_twin():
        return pltpu.make_async_remote_copy(
            own, m1.at[s], send_sem.at[32], recv_sem.at[s], device_id=(I, c + 1 - 2 * s, h), device_id_type=MESH
        )

    def to_hub(n):
        return pltpu.make_async_remote_copy(
            hubw, hub_i.at[s], hub_send.at[n], hub_recv.at[s], device_id=(I, n, h), device_id_type=MESH
        )

    def each_hub(act):
        @pl.when(diag)
        def _():
            for n in range(16):
                @pl.when(n != c)
                def _(n=n):
                    act(to_hub(n))

    def each_block(act):
        for n in range(16):
            @pl.when(bit_of(to_rows, n))
            def _(n=n):
                act(to_row(n))

        for n in range(16):
            @pl.when(bit_of(to_cols, n))
            def _(n=n):
                act(to_col(n))

        act(to_twin())

    each_hub(lambda d: d.start())
    each_block(lambda d: d.start())

    loads[2].wait()
    loads[3].wait()
    lane_w = lax.broadcasted_iota(jnp.int32, (8, 128), 1)
    sub_w = lax.broadcasted_iota(jnp.int32, (8, 128), 0)
    word_id = jnp.where(sub_w == 0, I * W, K * W) + lane_w
    word_id = jnp.where(lane_w < W, word_id, -1)
    col_id = J * B + lax.broadcasted_iota(jnp.int32, (16, 128), 0) * 128 + lax.broadcasted_iota(jnp.int32, (16, 128), 1)

    def mark(g, carry):
        words, flags = carry
        for n in range(16):
            v = ids_s[lax.div(g, 8), lax.rem(g, 8) * 16 + n]
            words = words | jnp.where(
                word_id == jnp.right_shift(v, 5), jnp.left_shift(jnp.int32(1), jnp.bitwise_and(v, 31)), 0
            )
            flags = flags | (col_id == v).astype(jnp.int32)
        return words, flags

    words, flags = lax.fori_loop(
        0, 16, mark, (jnp.zeros((8, 128), jnp.int32), jnp.zeros((16, 128), jnp.int32))
    )
    keep_words = jnp.bitwise_not(words)
    keep_i = jnp.broadcast_to(keep_words[0:1, :], (128, 128)).T[:W]
    keep_k = jnp.broadcast_to(keep_words[1:2, :], (128, 128)).T[:W]
    keep_col = flags - 1

    def keep_cols_of(half, t):
        n = C // 128
        return jnp.where(half == 0, keep_col[t : t + 1, :], keep_col[n + t : n + t + 1, :])

    def mask_half(half):
        for t in range(C // 128):
            at = slice(t * 128, t * 128 + 128)
            mm1[half, :, at] = m1[half, :, at] & keep_i & keep_cols_of(half, t)

    mask_half(s)
    unpack_into(o8, mm1.at[s], W)

    @pl.when(diag)
    def _():
        hub_i[s] = hubw[...]

    def hub_half(half):
        pltpu.make_async_copy(hubw, hub_i.at[half], hub_recv.at[half]).wait()

    @pl.when(off)
    def _():
        hub_half(s)

    hub_half(o)
    G = hubw.shape[0]
    for half in range(2):
        for n, bits in enumerate(rows_of_bits(hub_i[half], 0, G)):
            r8[n * 32 : n * 32 + 32, half * C : half * C + C] = bits.astype(F32).astype(F8)
    reach = jnp.dot(r8[...], o8[...], preferred_element_type=F32)
    edge = hubw[...]
    lanes_c = jnp.concatenate([keep_cols_of(s, t) for t in range(C // 128)], axis=1)
    edge = edge & lanes_c
    hub_bits = jnp.concatenate(rows_of_bits(edge, 0, G), axis=0)
    meet = jnp.where(hub_bits != 0, reach, 0.0)
    hub_flag = hub_bits.astype(F32)

    def across(x):
        t = x[:, 0:128]
        for n in range(1, x.shape[1] // 128):
            t = t + x[:, n * 128 : n * 128 + 128]
        return jnp.sum(t.T, axis=0, keepdims=True)

    hub_tri = 0.5 * across(meet)
    hub_deg = across(hub_flag)
    hpart[...] = hub_tri

    def to_column(n):
        return pltpu.make_async_remote_copy(
            hpart, h_in.at[I], ha_send.at[n], ha_recv.at[I], device_id=(n, c, h), device_id_type=MESH
        )

    def others(act):
        for n in range(8):
            @pl.when(n != I)
            def _(n=n):
                act(n)

    others(lambda n: to_column(n).start())

    light_deg = jnp.sum(lax.population_count(mm1[s]).astype(F32), axis=0, keepdims=True) * 0.5
    edge_deg = jnp.sum(lax.population_count(edge).astype(F32), axis=0, keepdims=True)
    col[0:1, :] = jnp.sum(meet, axis=0, keepdims=True)
    col[1:2, :] = light_deg + jnp.where(diag, 1.0, 0.0) * edge_deg

    def recv(ref, sem):
        pltpu.make_async_copy(own, ref, sem).wait()

    @pl.when(K != J)
    def _():
        recv(m2.at[0], recv_sem.at[2])
        recv(m2.at[1], recv_sem.at[3])

    @pl.when(K == J)
    def _():
        recv(m1.at[o], recv_sem.at[o])
        m2[...] = m1[...]

    unpack_into(a8, m2.at[0], W, 0)
    unpack_into(a8, m2.at[1], W, C)
    acc_r[...] = jnp.zeros_like(acc_r)
    row_w = jnp.where(diag, 0.125, jnp.where(K == I, 1.0, 0.5))
    col_w = jnp.where(diag, 0.0, jnp.where(K == J, 1.0, 0.5))
    MC, NC = 512, 256
    shift = lax.broadcasted_iota(jnp.int32, (32, NC), 0)

    def to_owner(n, k):
        return pltpu.make_async_remote_copy(
            cmsg.at[n],
            c_in.at[I * 4 + s * 2 + h],
            cs_sem.at[n * 2 + k],
            cr_sem.at[I * 4 + s * 2 + h],
            device_id=(J, n, k),
            device_id_type=MESH,
        )

    def face(half, name):
        @pl.when(K != I)
        def _():
            recv(m3.at[half], recv_sem.at[4 + half])

        @pl.when(K == I)
        def _():
            m3[half] = m1[half]

        for t in range(C // 128):
            at = slice(t * 128, t * 128 + 128)
            m3[half, :, at] = m3[half, :, at] & keep_k
        unpack_into(b8.at[half], m3.at[half], W)

        def chunk(n, carry):
            at = pl.multiple_of(n * NC, NC)
            sums = jnp.zeros((8, NC), F32)
            for m in range(B // MC):
                paths = jnp.dot(
                    a8[m * MC : m * MC + MC, :], b8[half, :, pl.ds(at, NC)], preferred_element_type=F32
                )
                for w in range(MC // 32):
                    word = m * (MC // 32) + w
                    x = jnp.broadcast_to(mm1[half, word : word + 1, pl.ds(at, NC)], (32, NC))
                    bits = jnp.bitwise_and(jnp.right_shift(x, shift), 1)
                    t = jnp.where(bits != 0, paths[w * 32 : w * 32 + 32], 0.0)
                    sums = sums + jnp.sum(t.reshape(4, 8, NC), axis=0)
                    acc_r[word * 32 : word * 32 + 32, :] += t[:, :128] + t[:, 128:]
            acc_c[:, pl.ds(at, NC)] = sums
            return carry

        lax.fori_loop(0, C // NC, chunk, 0)

    def send_cols(half, first):
        whole = col_w * jnp.sum(acc_c[...], axis=0, keepdims=True)
        if first:
            whole = whole + col[0:1, :]
        for k in range(C // V):
            n = half * (C // V) + k
            cmsg[n, 0:1, 0:V] = whole[:, k * V : k * V + V]
            if first:
                cmsg[n, 1:2, 0:V] = col[1:2, k * V : k * V + V]
            else:
                cmsg[n, 1:2, 0:V] = jnp.zeros((1, V), F32)
        for k in range(C // V):
            n = half * (C // V) + k
            for g in range(2):
                @pl.when(jnp.logical_or(off, jnp.logical_or(n != c, g != h)))
                def _(n=n, g=g):
                    to_owner(n, g).start()

    face(s, "p13")
    others(lambda n: pltpu.make_async_copy(hpart, h_in.at[n], ha_recv.at[n]).wait())
    h_in[I] = hpart[...]
    send_cols(s, True)
    @pl.when(K != J)
    def _():
        recv(m1.at[o], recv_sem.at[o])

    mask_half(o)
    face(o, "p16")
    send_cols(o, False)

    hub_all = h_in[0]
    for n in range(1, 8):
        hub_all = hub_all + h_in[n]
    for n in range(B // V):
        rmsg[n, 0:1, 0:V] = jnp.sum(acc_r[n * V : n * V + V, :].T, axis=0, keepdims=True) * row_w
        rmsg[n, 1:2, :] = hub_all
        rmsg[n, 2:3, :] = hub_deg

    def to_plane(n):
        return pltpu.make_async_remote_copy(
            rmsg.at[n // 2],
            r_in.at[me],
            rs_sem.at[n],
            rr_sem.at[me],
            device_id=(I, n // 2, n % 2),
            device_id_type=MESH,
        )

    def plane(act):
        for n in range(32):
            @pl.when(n != me)
            def _(n=n):
                act(n)

    plane(lambda n: to_plane(n).start())
    r_in[me] = rmsg[c]

    @pl.when(diag)
    def _():
        c_in[I * 4 + s * 2 + h] = cmsg[c]

    vertex = I * B + c * V + lax.broadcasted_iota(jnp.int32, (V, 128), 0)
    is_hub = [vertex == ids_v[g : g + 1, :] for g in range(2)]
    each_hub(lambda d: d.wait_send())
    each_block(lambda d: d.wait_send())
    others(lambda n: to_column(n).wait_send())

    def wait_cols(n):
        pltpu.make_async_copy(cmsg.at[0], c_in.at[n], cr_sem.at[n]).wait()

    for n in range(32):
        @pl.when(jnp.logical_or(off, n != I * 4 + s * 2 + h))
        def _(n=n):
            wait_cols(n)

    plane(lambda n: pltpu.make_async_copy(rmsg.at[0], r_in.at[n], rr_sem.at[n]).wait())
    even = r_in[0]
    odd = r_in[1]
    for n in range(1, 16):
        even = even + r_in[2 * n]
        odd = odd + r_in[2 * n + 1]
    both = even + odd
    cols = c_in[0]
    for n in range(1, 32):
        cols = cols + c_in[n]

    def at_hubs(r):
        rows = [jnp.broadcast_to(x[r : r + 1, :], (V, 128)) for x in (even, odd)]
        hit = jnp.where(is_hub[0], rows[0], 0.0) + jnp.where(is_hub[1], rows[1], 0.0)
        return jnp.sum(hit.T, axis=0, keepdims=True)

    tri = both[0:1, :V] + cols[0:1, :V] + at_hubs(1)
    deg = cols[1:2, :V] + at_hubs(2)
    out[...] = tri / (1.0 + deg)
    for n in range(B // V):
        for g in range(2):
            @pl.when(jnp.logical_or(off, jnp.logical_or(n != c, g != h)))
            def _(n=n, g=g):
                to_owner(n, g).wait_send()

    plane(lambda n: to_plane(n).wait_send())


ROWS_TO, COLS_TO = destinations()


def body(light_bits, hub_bits, hub_ids):
    W, C = light_bits.shape
    G = hub_bits.shape[0]
    B = 2 * C
    V = B // 16
    vmem = pl.BlockSpec(memory_space=pltpu.VMEM)
    out = pl.pallas_call(
        kernel,
        out_shape=jax.ShapeDtypeStruct((1, V), F32),
        in_specs=[pl.BlockSpec(memory_space=pltpu.HBM)] * 3,
        out_specs=vmem,
        scratch_shapes=[
            pltpu.SMEM((2, 128), jnp.int32),
            pltpu.VMEM((2, 128), jnp.int32),
            pltpu.VMEM((2, W, C), jnp.int32),
            pltpu.VMEM((2, W, C), jnp.int32),
            pltpu.VMEM((2, W, C), jnp.int32),
            pltpu.VMEM((2, W, C), jnp.int32),
            pltpu.VMEM((G, C), jnp.int32),
            pltpu.VMEM((2, G, C), jnp.int32),
            pltpu.VMEM((B, B), F8),
            pltpu.VMEM((2, B, C), F8),
            pltpu.VMEM((B, C), F8),
            pltpu.VMEM((32 * G, B), F8),
            pltpu.VMEM((B, 128), F32),
            pltpu.VMEM((8, C), F32),
            pltpu.VMEM((2, C), F32),
            pltpu.VMEM((1, 128), F32),
            pltpu.VMEM((8, 1, 128), F32),
            pltpu.VMEM((16, 4, 128), F32),
            pltpu.VMEM((16, 2, 128), F32),
            pltpu.VMEM((32, 4, 128), F32),
            pltpu.VMEM((32, 2, 128), F32),
            pltpu.SemaphoreType.DMA((4,)),
            pltpu.SemaphoreType.DMA((33,)),
            pltpu.SemaphoreType.DMA((6,)),
            pltpu.SemaphoreType.DMA((16,)),
            pltpu.SemaphoreType.DMA((2,)),
            pltpu.SemaphoreType.DMA((8,)),
            pltpu.SemaphoreType.DMA((8,)),
            pltpu.SemaphoreType.DMA((32,)),
            pltpu.SemaphoreType.DMA((32,)),
            pltpu.SemaphoreType.DMA((32,)),
            pltpu.SemaphoreType.DMA((32,)),
        ],
        compiler_params=pltpu.CompilerParams(
            collective_id=0, has_side_effects=True, vmem_limit_bytes=67043328
        ),
    )(light_bits, hub_bits, hub_ids.reshape(2, 128))
    return out.reshape(V)


def solution(mesh):
    placed = (P("rows", "cols"), P("hub", "cols"), P())
    return jax.shard_map(body, mesh=mesh, in_specs=placed, out_specs=P(("rows", "cols")), check_vma=False)
```

```python
import functools

import jax
import jax.numpy as jnp
from jax import lax
from jax.experimental import pallas as pl
from jax.experimental.pallas import tpu as pltpu
from jax.sharding import PartitionSpec as P

MESH = pl.DeviceIdType.MESH
F32 = jnp.float32
F8 = jnp.float8_e4m3fn

THIRD = [
    0, 0, 47, 3, 42, 35, 59, 41, 28, 46, 60, 43, 52, 59, 46, 23,
    52, 17, 9, 9, 22, 4, 37, 26, 53, 34, 47, 20, 39, 22, 53, 59,
    62, 1, 11, 47, 18, 18, 17, 61, 4, 61, 33, 47, 48, 15, 37, 55,
    48, 20, 62, 1, 3, 38, 27, 27, 40, 52, 13, 52, 47, 52, 14, 56,
    15, 2, 25, 7, 11, 22, 11, 23, 36, 36, 25, 60, 62, 1, 59, 41,
    16, 49, 48, 11, 16, 51, 24, 58, 2, 46, 45, 45, 20, 48, 14, 7,
    13, 2, 13, 24, 35, 21, 1, 19, 42, 35, 43, 57, 54, 54, 46, 11,
    32, 25, 32, 17, 8, 26, 26, 44, 22, 4, 26, 44, 60, 16, 63, 63,
]


def nearer(j, k, h):
    here = j // 2 * 2 + h

    def hops(g):
        d = (k // 2 * 2 + g - here) % 8
        return min(d, 8 - d)

    return 1 - h if hops(1 - h) < hops(h) else h


def destinations():
    rows, cols = ([0] * 128, [0] * 128), [0] * 128
    for i in range(8):
        for j in range(8):
            for h in range(2):
                for s in range(2):
                    k = THIRD[(i * 8 + j) * 2 + h] >> (3 * s) & 7
                    if i != j and k != j:
                        rows[h][(i * 8 + k) * 2 + nearer(j, k, h)] |= 1 << (2 * j + s)
                    if i != j and k != i:
                        cols[(k * 8 + j) * 2 + h] |= 1 << (2 * i + s)
    return rows[0], rows[1], cols


def lookup(tables, index, bits):
    tables = [list(t) for t in tables]
    for b in range(bits):
        odd = lax.rem(lax.div(index, 2**b), 2) == 1
        tables = [
            [x if isinstance(x, int) and x is y else jnp.where(odd, y, x) for x, y in zip(t[0::2], t[1::2])]
            for t in tables
        ]
    return [t[0] for t in tables]


def bit_of(mask, n):
    return lax.rem(lax.div(mask, 2**n), 2) == 1


def rows_of_bits(words, first, count):
    shift = lax.broadcasted_iota(jnp.int32, (32, words.shape[1]), 0)
    spread = [jnp.broadcast_to(words[w : w + 1, :], shift.shape) for w in range(first, first + count)]
    return [jnp.bitwise_and(jnp.right_shift(x, shift), 1) for x in spread]


def unpack_into(dst, src, words, lane=0):
    width = src.shape[1]

    def step(g, carry):
        block = src[pl.ds(pl.multiple_of(g * 8, 8), 8), :]
        for n, bits in enumerate(rows_of_bits(block, 0, 8)):
            at = pl.multiple_of(g * 256 + n * 32, 32)
            dst[pl.ds(at, 32), lane : lane + width] = bits.astype(F32).astype(dst.dtype)
        return carry

    lax.fori_loop(0, words // 8, step, 0)


def kernel(
    lb, hb, ids, out,
    ids_s, ids_v, m1, m2, m3, mm1, hubw, hub_i, a8, b8, o8, r8,
    acc_r, acc_c, col, hpart, h_in, rmsg, cmsg, r_in, c_in,
    local_sem, send_sem, recv_sem, hub_send, hub_recv, ha_send, ha_recv, rs_sem, rr_sem, cs_sem, cr_sem,
):
    I = lax.axis_index("rows")
    c = lax.axis_index("cols")
    h = lax.axis_index("hub")
    J = lax.div(c, 2)
    s = lax.rem(c, 2)
    o = 1 - s
    W = m1.shape[1]
    C = m1.shape[2]
    B = 2 * C
    V = out.shape[1]
    diag = I == J
    off = jnp.logical_not(diag)

    loads = [
        pltpu.make_async_copy(lb, m1.at[s], local_sem.at[0]),
        pltpu.make_async_copy(hb, hubw, local_sem.at[1]),
        pltpu.make_async_copy(ids, ids_s, local_sem.at[2]),
        pltpu.make_async_copy(ids, ids_v, local_sem.at[3]),
    ]
    for load in loads:
        load.start()

    barrier = pltpu.get_barrier_semaphore()

    def signal(dev):
        pl.semaphore_signal(barrier, inc=1, device_id=dev, device_id_type=MESH)

    me = c * 2 + h
    for n in range(1, 32):
        peer = lax.rem(me + n, 32)
        signal((I, lax.div(peer, 2), lax.rem(peer, 2)))
    for n in range(1, 8):
        for half in range(2):
            signal((lax.rem(I + n, 8), 2 * J + half, h))

    to_rows0, to_rows1, to_cols, thirds = lookup([ROWS0_TO, ROWS1_TO, COLS_TO, THIRD], (I * 8 + J) * 2 + h, 7)
    K = lax.rem(jnp.where(s == 1, lax.div(thirds, 8), thirds), 8)
    K_twin = lax.rem(jnp.where(s == 0, lax.div(thirds, 8), thirds), 8)
    loads[0].wait()
    loads[1].wait()
    pl.semaphore_wait(barrier, 45)

    own = m1.at[s]

    def to_row(n, g, sem):
        return pltpu.make_async_remote_copy(
            own, m2.at[s], send_sem.at[sem], recv_sem.at[2 + s], device_id=(I, n, g), device_id_type=MESH
        )

    def to_col(n, sem):
        return pltpu.make_async_remote_copy(
            own,
            m3.at[s],
            send_sem.at[sem],
            recv_sem.at[4 + s],
            device_id=(n // 2, 2 * J + n % 2, h),
            device_id_type=MESH,
        )

    def to_twin():
        return pltpu.make_async_remote_copy(
            own, m1.at[s], send_sem.at[0], recv_sem.at[s], device_id=(I, c + 1 - 2 * s, h), device_id_type=MESH
        )

    def to_hub(n):
        return pltpu.make_async_remote_copy(
            hubw, hub_i.at[s], hub_send.at[n], hub_recv.at[s], device_id=(I, n, h), device_id_type=MESH
        )

    def each_hub(act):
        @pl.when(diag)
        def _():
            for n in range(16):
                @pl.when(n != c)
                def _(n=n):
                    act(to_hub(n))

    each_hub(lambda d: d.start())
    sent = jnp.int32(1)
    for g, mask in enumerate((to_rows0, to_rows1)):
        for n in range(16):
            go = bit_of(mask, n)

            @pl.when(go)
            def _(n=n, g=g, sent=sent):
                to_row(n, g, sent).start()

            sent = sent + go.astype(jnp.int32)

    for n in range(16):
        go = jnp.logical_and(bit_of(to_cols, n), s == n % 2)

        @pl.when(go)
        def _(n=n, sent=sent):
            to_col(n, sent).start()

        sent = sent + go.astype(jnp.int32)

    @pl.when(K_twin == J)
    def _():
        to_twin().start()

    loads[2].wait()
    loads[3].wait()
    lane_w = lax.broadcasted_iota(jnp.int32, (8, 128), 1)
    sub_w = lax.broadcasted_iota(jnp.int32, (8, 128), 0)
    word_id = jnp.where(sub_w == 0, I * W, K * W) + lane_w
    word_id = jnp.where(lane_w < W, word_id, -1)
    col_id = J * B + lax.broadcasted_iota(jnp.int32, (16, 128), 0) * 128 + lax.broadcasted_iota(jnp.int32, (16, 128), 1)

    def mark(g, carry):
        words, flags = carry
        for n in range(16):
            v = ids_s[lax.div(g, 8), lax.rem(g, 8) * 16 + n]
            words = words | jnp.where(
                word_id == jnp.right_shift(v, 5), jnp.left_shift(jnp.int32(1), jnp.bitwise_and(v, 31)), 0
            )
            flags = flags | (col_id == v).astype(jnp.int32)
        return words, flags

    words, flags = lax.fori_loop(
        0, 16, mark, (jnp.zeros((8, 128), jnp.int32), jnp.zeros((16, 128), jnp.int32))
    )
    keep_words = jnp.bitwise_not(words)
    keep_i = jnp.broadcast_to(keep_words[0:1, :], (128, 128)).T[:W]
    keep_k = jnp.broadcast_to(keep_words[1:2, :], (128, 128)).T[:W]
    keep_col = flags - 1

    def keep_cols_of(half, t):
        n = C // 128
        return jnp.where(half == 0, keep_col[t : t + 1, :], keep_col[n + t : n + t + 1, :])

    def mask_half(half):
        for t in range(C // 128):
            at = slice(t * 128, t * 128 + 128)
            mm1[half, :, at] = m1[half, :, at] & keep_i & keep_cols_of(half, t)

    mask_half(s)
    unpack_into(o8, mm1.at[s], W)

    @pl.when(diag)
    def _():
        hub_i[s] = hubw[...]

    def hub_half(half):
        pltpu.make_async_copy(hubw, hub_i.at[half], hub_recv.at[half]).wait()

    @pl.when(off)
    def _():
        hub_half(s)

    hub_half(o)
    G = hubw.shape[0]
    for half in range(2):
        for n, bits in enumerate(rows_of_bits(hub_i[half], 0, G)):
            r8[n * 32 : n * 32 + 32, half * C : half * C + C] = bits.astype(F32).astype(F8)
    reach = jnp.dot(r8[...], o8[...], preferred_element_type=F32)
    edge = hubw[...]
    lanes_c = jnp.concatenate([keep_cols_of(s, t) for t in range(C // 128)], axis=1)
    edge = edge & lanes_c
    hub_bits = jnp.concatenate(rows_of_bits(edge, 0, G), axis=0)
    meet = jnp.where(hub_bits != 0, reach, 0.0)
    hub_flag = hub_bits.astype(F32)

    def across(x):
        t = x[:, 0:128]
        for n in range(1, x.shape[1] // 128):
            t = t + x[:, n * 128 : n * 128 + 128]
        return jnp.sum(t.T, axis=0, keepdims=True)

    hub_tri = 0.5 * across(meet)
    hub_deg = across(hub_flag)
    hpart[...] = hub_tri

    def to_column(n):
        return pltpu.make_async_remote_copy(
            hpart, h_in.at[I], ha_send, ha_recv, device_id=(n, c, h), device_id_type=MESH
        )

    def others(act):
        for n in range(8):
            @pl.when(n != I)
            def _(n=n):
                act(n)

    others(lambda n: to_column(n).start())

    light_deg = jnp.sum(lax.population_count(mm1[s]).astype(F32), axis=0, keepdims=True) * 0.5
    edge_deg = jnp.sum(lax.population_count(edge).astype(F32), axis=0, keepdims=True)
    col[0:1, :] = jnp.sum(meet, axis=0, keepdims=True)
    col[1:2, :] = light_deg + jnp.where(diag, 1.0, 0.0) * edge_deg

    def recv(ref, sem):
        pltpu.make_async_copy(own, ref, sem).wait()

    for n in range(16):
        go = jnp.logical_and(bit_of(to_cols, n), s != n % 2)

        @pl.when(go)
        def _(n=n, sent=sent):
            to_col(n, sent).start()

        sent = sent + go.astype(jnp.int32)

    @pl.when(K_twin != J)
    def _():
        to_twin().start()

    @pl.when(K != J)
    def _():
        recv(m2.at[0], recv_sem.at[2])

    @pl.when(K == J)
    def _():
        recv(m1.at[o], recv_sem.at[o])
        m2[...] = m1[...]

    unpack_into(a8, m2.at[0], W, 0)
    @pl.when(K != J)
    def _():
        recv(m2.at[1], recv_sem.at[3])

    unpack_into(a8, m2.at[1], W, C)
    acc_r[...] = jnp.zeros_like(acc_r)
    row_w = jnp.where(diag, 0.125, jnp.where(K == I, 1.0, 0.5))
    col_w = jnp.where(diag, 0.0, jnp.where(K == J, 1.0, 0.5))
    MC = 256
    shift = lax.broadcasted_iota(jnp.int32, (32, C), 0)

    def to_owner(n, k):
        return pltpu.make_async_remote_copy(
            cmsg.at[n],
            c_in.at[I * 4 + s * 2 + h],
            cs_sem,
            cr_sem,
            device_id=(J, n, k),
            device_id_type=MESH,
        )

    def face(half, name):
        @pl.when(K != I)
        def _():
            recv(m3.at[half], recv_sem.at[4 + half])

        @pl.when(K == I)
        def _():
            m3[half] = m1[half]

        for t in range(C // 128):
            at = slice(t * 128, t * 128 + 128)
            m3[half, :, at] = m3[half, :, at] & keep_k
        unpack_into(b8.at[half], m3.at[half], W)

        acc_c[...] = jnp.zeros_like(acc_c)

        def chunk(g, carry):
            sums = acc_c[...]
            for u in range(2):
                m = g * 2 + u
                paths = jnp.dot(
                    a8[pl.ds(pl.multiple_of(m * MC, MC), MC), :], b8[half], preferred_element_type=F32
                )
                words = mm1[half, pl.ds(pl.multiple_of(m * (MC // 32), MC // 32), MC // 32), :]
                for w in range(MC // 32):
                    x = jnp.broadcast_to(words[w : w + 1, :], (32, C))
                    bits = jnp.bitwise_and(jnp.right_shift(x, shift), 1)
                    t = jnp.where(bits != 0, paths[w * 32 : w * 32 + 32], 0.0)
                    sums = sums + jnp.sum(t.reshape(4, 8, C), axis=0)
                    row = t[:, 0:128]
                    for q in range(1, C // 128):
                        row = row + t[:, q * 128 : q * 128 + 128]
                    acc_r[pl.ds(pl.multiple_of(m * MC + w * 32, 32), 32), :] += row
            acc_c[...] = sums
            return carry

        lax.fori_loop(0, B // (2 * MC), chunk, 0)

    def send_cols(half, first):
        whole = col_w * jnp.sum(acc_c[...], axis=0, keepdims=True)
        if first:
            whole = whole + col[0:1, :]
        for k in range(C // V):
            n = half * (C // V) + k
            cmsg[n, 0:1, 0:V] = whole[:, k * V : k * V + V]
            if first:
                cmsg[n, 1:2, 0:V] = col[1:2, k * V : k * V + V]
            else:
                cmsg[n, 1:2, 0:V] = jnp.zeros((1, V), F32)
        for k in range(C // V):
            n = half * (C // V) + k
            for g in range(2):
                @pl.when(jnp.logical_or(off, jnp.logical_or(n != c, g != h)))
                def _(n=n, g=g):
                    to_owner(n, g).start()

    face(s, "p13")
    pltpu.make_async_copy(h_in.at[pl.ds(0, 7)], h_in.at[pl.ds(0, 7)], ha_recv).wait()
    h_in[I] = hpart[...]
    send_cols(s, True)
    @pl.when(K != J)
    def _():
        recv(m1.at[o], recv_sem.at[o])

    mask_half(o)
    face(o, "p16")
    send_cols(o, False)

    hub_all = h_in[0]
    for n in range(1, 8):
        hub_all = hub_all + h_in[n]
    for n in range(B // V):
        rmsg[n, 0:1, 0:V] = jnp.sum(acc_r[n * V : n * V + V, :].T, axis=0, keepdims=True) * row_w
        rmsg[n, 1:2, :] = hub_all
        rmsg[n, 2:3, :] = hub_deg

    def to_plane(n):
        return pltpu.make_async_remote_copy(
            rmsg.at[n // 2],
            r_in.at[me],
            rs_sem,
            rr_sem,
            device_id=(I, n // 2, n % 2),
            device_id_type=MESH,
        )

    def plane(act):
        for n in range(32):
            @pl.when(n != me)
            def _(n=n):
                act(n)

    plane(lambda n: to_plane(n).start())
    r_in[me] = rmsg[c]

    @pl.when(diag)
    def _():
        c_in[I * 4 + s * 2 + h] = cmsg[c]

    vertex = I * B + c * V + lax.broadcasted_iota(jnp.int32, (V, 128), 0)
    is_hub = [vertex == ids_v[g : g + 1, :] for g in range(2)]
    each_hub(lambda d: d.wait_send())
    for n in range(MOST_SENDS):
        @pl.when(n < sent)
        def _(n=n):
            pltpu.make_async_copy(own, m2.at[s], send_sem.at[n]).wait()

    pltpu.make_async_copy(h_in.at[pl.ds(0, 7)], h_in.at[pl.ds(0, 7)], ha_send).wait()

    def wait_slots(ref, sem, count):
        part = ref.at[pl.ds(0, count)]
        pltpu.make_async_copy(part, part, sem).wait()

    def wait_cols(sem):
        @pl.when(off)
        def _():
            wait_slots(c_in, sem, 32)

        @pl.when(diag)
        def _():
            wait_slots(c_in, sem, 31)

    wait_cols(cr_sem)
    wait_slots(r_in, rr_sem, 31)
    even = r_in[0]
    odd = r_in[1]
    for n in range(1, 16):
        even = even + r_in[2 * n]
        odd = odd + r_in[2 * n + 1]
    both = even + odd
    cols = c_in[0]
    for n in range(1, 32):
        cols = cols + c_in[n]

    def at_hubs(r):
        rows = [jnp.broadcast_to(x[r : r + 1, :], (V, 128)) for x in (even, odd)]
        hit = jnp.where(is_hub[0], rows[0], 0.0) + jnp.where(is_hub[1], rows[1], 0.0)
        return jnp.sum(hit.T, axis=0, keepdims=True)

    tri = both[0:1, :V] + cols[0:1, :V] + at_hubs(1)
    deg = cols[1:2, :V] + at_hubs(2)
    out[...] = tri / (1.0 + deg)
    wait_cols(cs_sem)
    wait_slots(r_in, rs_sem, 31)


ROWS0_TO, ROWS1_TO, COLS_TO = destinations()
MOST_SENDS = 1 + max(sum(bin(m).count("1") for m in masks) for masks in zip(ROWS0_TO, ROWS1_TO, COLS_TO))


def body(light_bits, hub_bits, hub_ids):
    W, C = light_bits.shape
    G = hub_bits.shape[0]
    B = 2 * C
    V = B // 16
    vmem = pl.BlockSpec(memory_space=pltpu.VMEM)
    out = pl.pallas_call(
        kernel,
        out_shape=jax.ShapeDtypeStruct((1, V), F32),
        in_specs=[pl.BlockSpec(memory_space=pltpu.HBM)] * 3,
        out_specs=vmem,
        scratch_shapes=[
            pltpu.SMEM((2, 128), jnp.int32),
            pltpu.VMEM((2, 128), jnp.int32),
            pltpu.VMEM((2, W, C), jnp.int32),
            pltpu.VMEM((2, W, C), jnp.int32),
            pltpu.VMEM((2, W, C), jnp.int32),
            pltpu.VMEM((2, W, C), jnp.int32),
            pltpu.VMEM((G, C), jnp.int32),
            pltpu.VMEM((2, G, C), jnp.int32),
            pltpu.VMEM((B, B), F8),
            pltpu.VMEM((2, B, C), F8),
            pltpu.VMEM((B, C), F8),
            pltpu.VMEM((32 * G, B), F8),
            pltpu.VMEM((B, 128), F32),
            pltpu.VMEM((8, C), F32),
            pltpu.VMEM((2, C), F32),
            pltpu.VMEM((1, 128), F32),
            pltpu.VMEM((8, 1, 128), F32),
            pltpu.VMEM((16, 4, 128), F32),
            pltpu.VMEM((16, 2, 128), F32),
            pltpu.VMEM((32, 4, 128), F32),
            pltpu.VMEM((32, 2, 128), F32),
            pltpu.SemaphoreType.DMA((4,)),
            pltpu.SemaphoreType.DMA((MOST_SENDS,)),
            pltpu.SemaphoreType.DMA((6,)),
            pltpu.SemaphoreType.DMA((16,)),
            pltpu.SemaphoreType.DMA((2,)),
            pltpu.SemaphoreType.DMA,
            pltpu.SemaphoreType.DMA,
            pltpu.SemaphoreType.DMA,
            pltpu.SemaphoreType.DMA,
            pltpu.SemaphoreType.DMA,
            pltpu.SemaphoreType.DMA,
        ],
        compiler_params=pltpu.CompilerParams(
            collective_id=0, has_side_effects=True, vmem_limit_bytes=67043328
        ),
    )(light_bits, hub_bits, hub_ids.reshape(2, 128))
    return out.reshape(V)


def solution(mesh):
    placed = (P("rows", "cols"), P("hub", "cols"), P())
    return jax.shard_map(body, mesh=mesh, in_specs=placed, out_specs=P(("rows", "cols")), check_vma=False)
```

```python
import functools

import jax
import jax.numpy as jnp
from jax import lax
from jax.experimental import pallas as pl
from jax.experimental.pallas import tpu as pltpu
from jax.sharding import PartitionSpec as P

MESH = pl.DeviceIdType.MESH
F32 = jnp.float32
F8 = jnp.float8_e4m3fn

THIRD = [
    0, 0, 43, 57, 26, 55, 15, 43, 13, 35, 47, 11, 20, 62, 41, 31,
    16, 52, 9, 9, 38, 16, 21, 28, 34, 6, 2, 46, 52, 2, 60, 53,
    13, 32, 11, 47, 18, 18, 13, 31, 48, 39, 57, 29, 40, 55, 47, 25,
    50, 4, 57, 6, 6, 20, 27, 27, 12, 2, 20, 46, 48, 20, 10, 60,
    22, 7, 31, 13, 26, 13, 47, 51, 36, 36, 26, 47, 51, 40, 51, 57,
    48, 34, 33, 59, 4, 50, 3, 15, 32, 49, 45, 45, 22, 4, 8, 31,
    8, 29, 29, 57, 33, 26, 31, 41, 15, 34, 61, 11, 54, 54, 31, 41,
    20, 48, 1, 19, 2, 52, 51, 5, 20, 5, 22, 44, 32, 50, 63, 63,
]


def nearer(j, k, h):
    here = j // 2 * 2 + h

    def hops(g):
        d = (k // 2 * 2 + g - here) % 8
        return min(d, 8 - d)

    return 1 - h if hops(1 - h) < hops(h) else h


def destinations():
    rows, cols = ([0] * 128, [0] * 128), [0] * 128
    for i in range(8):
        for j in range(8):
            for h in range(2):
                for s in range(2):
                    k = THIRD[(i * 8 + j) * 2 + h] >> (3 * s) & 7
                    if i != j and k != j:
                        rows[h][(i * 8 + k) * 2 + nearer(j, k, h)] |= 1 << (2 * j + s)
                    if i != j and k != i:
                        cols[((k * 8 + j) * 2 + h)] |= 1 << (8 * s + i)
    return rows[0], rows[1], cols


def lookup(tables, index, bits):
    tables = [list(t) for t in tables]
    for b in range(bits):
        odd = lax.rem(lax.div(index, 2**b), 2) == 1
        tables = [
            [x if isinstance(x, int) and x is y else jnp.where(odd, y, x) for x, y in zip(t[0::2], t[1::2])]
            for t in tables
        ]
    return [t[0] for t in tables]


def bit_of(mask, n):
    return lax.rem(lax.div(mask, 2**n), 2) == 1


def rows_of_bits(words, first, count):
    shift = lax.broadcasted_iota(jnp.int32, (32, words.shape[1]), 0)
    spread = [jnp.broadcast_to(words[w : w + 1, :], shift.shape) for w in range(first, first + count)]
    return [jnp.bitwise_and(jnp.right_shift(x, shift), 1) for x in spread]


def unpack_into(dst, src, words, lane=0):
    width = src.shape[1]

    def step(g, carry):
        block = src[pl.ds(pl.multiple_of(g * 8, 8), 8), :]
        for n, bits in enumerate(rows_of_bits(block, 0, 8)):
            at = pl.multiple_of(g * 256 + n * 32, 32)
            dst[pl.ds(at, 32), lane : lane + width] = bits.astype(F32).astype(dst.dtype)
        return carry

    lax.fori_loop(0, words // 8, step, 0)


def kernel(
    lb, hb, ids, out,
    ids_s, ids_v, m1, m2, m3, mm1, hubw, hub_i, a0, a1, a2, a3, a4, a5, b_own, b_other, o8, r8,
    acc_r, col, hpart, h_in, rmsg, cmsg, r_in, c_in,
    local_sem, send_sem, recv_sem, hub_send, hub_recv, ha_send, ha_recv, rs_sem, rr_sem, cs_sem, cr_sem,
):
    I = lax.axis_index("rows")
    c = lax.axis_index("cols")
    h = lax.axis_index("hub")
    J = lax.div(c, 2)
    s = lax.rem(c, 2)
    o = 1 - s
    W = m1.shape[1]
    C = m1.shape[2]
    B = 2 * C
    V = out.shape[1]
    diag = I == J
    off = jnp.logical_not(diag)
    me = c * 2 + h

    loads = [
        pltpu.make_async_copy(lb, m1.at[s], local_sem.at[0]),
        pltpu.make_async_copy(hb, hubw, local_sem.at[1]),
        pltpu.make_async_copy(ids, ids_s, local_sem.at[2]),
        pltpu.make_async_copy(ids, ids_v, local_sem.at[3]),
    ]
    for load in loads:
        load.start()

    (thirds,) = lookup([THIRD], (I * 8 + J) * 2 + h, 7)
    K = lax.rem(jnp.where(s == 1, lax.div(thirds, 8), thirds), 8)
    ahead = lax.rem(lax.div(K, 2) - lax.div(J, 2) + 4, 4)
    near = jnp.where(ahead == 0, h, jnp.where(ahead == 1, 0, jnp.where(ahead == 3, 1, 1 - h)))

    barrier = pltpu.get_barrier_semaphore()

    def signal(dev):
        pl.semaphore_signal(barrier, inc=1, device_id=dev, device_id_type=MESH)

    signal((I, c + 1 - 2 * s, h))

    @pl.when(jnp.logical_and(off, K != J))
    def _():
        for x in range(2):
            signal((I, 2 * K + x, near))

    @pl.when(jnp.logical_and(off, K != I))
    def _():
        signal((K, c, h))

    for n in range(1, 8):
        signal((lax.rem(I + n, 8), c, h))
    for x in range(2):
        for g in range(2):
            @pl.when(jnp.logical_or(off, jnp.logical_or(s != x, h != g)))
            def _(x=x, g=g):
                signal((I, 2 * I + x, g))

    to_rows0, to_rows1, to_cols = lookup([ROWS0_TO, ROWS1_TO, COLS_TO], (I * 8 + J) * 2 + h, 7)
    to_cols = lax.rem(jnp.where(s == 1, lax.div(to_cols, 256), to_cols), 256)
    readers = 0
    for mask, count in ((to_rows0, 16), (to_rows1, 16), (to_cols, 8)):
        for n in range(count):
            readers = readers + lax.rem(lax.div(mask, 2**n), 2)
    greeted = readers + jnp.where(diag, 39, 8)
    loads[0].wait()
    loads[1].wait()
    pl.semaphore_wait(barrier, greeted)

    own = m1.at[s]

    def to_row(n, g, sem):
        return pltpu.make_async_remote_copy(
            own, m2.at[s], send_sem.at[sem], recv_sem.at[2 + s], device_id=(I, n, g), device_id_type=MESH
        )

    def to_col(n, half, sem):
        return pltpu.make_async_remote_copy(
            m1.at[half],
            m3.at[half],
            send_sem.at[sem],
            recv_sem.at[4 + half],
            device_id=(n, c, h),
            device_id_type=MESH,
        )

    def to_twin():
        return pltpu.make_async_remote_copy(
            own, m1.at[s], send_sem.at[0], recv_sem.at[s], device_id=(I, c + 1 - 2 * s, h), device_id_type=MESH
        )

    def to_hub(n):
        return pltpu.make_async_remote_copy(
            hubw, hub_i.at[s], hub_send.at[n], hub_recv.at[s], device_id=(I, n, h), device_id_type=MESH
        )

    def each_hub(act):
        @pl.when(diag)
        def _():
            for n in range(16):
                @pl.when(n != c)
                def _(n=n):
                    act(to_hub(n))

    each_hub(lambda d: d.start())
    to_twin().start()
    sent = jnp.int32(1)
    for n in range(8):
        go = bit_of(to_cols, n)

        @pl.when(go)
        def _(n=n, sent=sent):
            to_col(n, s, sent).start()

        sent = sent + go.astype(jnp.int32)

    for g, mask in enumerate((to_rows0, to_rows1)):
        for n in range(16):
            go = bit_of(mask, n)

            @pl.when(go)
            def _(n=n, g=g, sent=sent):
                to_row(n, g, sent).start()

            sent = sent + go.astype(jnp.int32)

    loads[2].wait()
    loads[3].wait()
    lane_w = lax.broadcasted_iota(jnp.int32, (8, 128), 1)
    sub_w = lax.broadcasted_iota(jnp.int32, (8, 128), 0)
    word_id = jnp.where(sub_w == 0, I * W, K * W) + lane_w
    word_id = jnp.where(lane_w < W, word_id, -1)
    col_id = J * B + lax.broadcasted_iota(jnp.int32, (16, 128), 0) * 128 + lax.broadcasted_iota(jnp.int32, (16, 128), 1)

    def mark(g, carry):
        words, flags = carry
        for n in range(16):
            v = ids_s[lax.div(g, 8), lax.rem(g, 8) * 16 + n]
            words = words | jnp.where(
                word_id == jnp.right_shift(v, 5), jnp.left_shift(jnp.int32(1), jnp.bitwise_and(v, 31)), 0
            )
            flags = flags | (col_id == v).astype(jnp.int32)
        return words, flags

    words, flags = lax.fori_loop(
        0, 16, mark, (jnp.zeros((8, 128), jnp.int32), jnp.zeros((16, 128), jnp.int32))
    )
    keep_words = jnp.bitwise_not(words)
    keep_i = jnp.broadcast_to(keep_words[0:1, :], (128, 128)).T[:W]
    keep_k = jnp.broadcast_to(keep_words[1:2, :], (128, 128)).T[:W]
    keep_k_wide = jnp.concatenate([keep_k] * (C // 128), axis=1)
    keep_col = flags - 1

    def keep_cols_of(half, t):
        n = C // 128
        return jnp.where(half == 0, keep_col[t : t + 1, :], keep_col[n + t : n + t + 1, :])

    def mask_half(half):
        for t in range(C // 128):
            at = slice(t * 128, t * 128 + 128)
            mm1[half, :, at] = m1[half, :, at] & keep_i & keep_cols_of(half, t)

    mask_half(s)
    unpack_into(o8, mm1.at[s], W)

    def recv(ref, sem):
        pltpu.make_async_copy(own, ref, sem).wait()

    rows_ik = (a0, a1, a2, a3, a4, a5)
    row_w = jnp.where(diag, 0.125, jnp.where(K == I, 1.0, 0.5))
    col_w = jnp.where(diag, 0.0, jnp.where(K == J, 1.0, 0.5))
    MC = 256

    def to_owner(n, k):
        return pltpu.make_async_remote_copy(
            cmsg.at[n],
            c_in.at[I * 4 + s * 2 + h],
            cs_sem,
            cr_sem,
            device_id=(J, n, k),
            device_id_type=MESH,
        )

    def kj(half, name):
        @pl.when(K != I)
        def _():
            recv(m3.at[half], recv_sem.at[4 + half])

        @pl.when(K == I)
        def _():
            m3[half] = m1[half]


    def kj_words(dst, half, first, count):
        for g in range(first, first + count, 8):
            words = m3[half, g : g + 8, :] & keep_k_wide[g : g + 8, :]
            for n, bits in enumerate(rows_of_bits(words, 0, 8)):
                dst[(g + n) * 32 : (g + n) * 32 + 32, :] = bits.astype(F32).astype(F8)

    def ik_rows(m):
        for half in range(2):
            words = m2[half, m * 8 : m * 8 + 8, :]
            for n, bits in enumerate(rows_of_bits(words, 0, 8)):
                rows_ik[m][n * 32 : n * 32 + 32, half * C : half * C + C] = bits.astype(F32).astype(F8)

    def product(m, b8, half, first, beside):
        paths = jnp.dot(rows_ik[m][...], b8[...], preferred_element_type=F32)
        beside()
        words = mm1[half, m * 8 : m * 8 + 8, :]
        sums = jnp.zeros((8, C), F32)
        for w, bits in enumerate(rows_of_bits(words, 0, 8)):
            t = jnp.where(bits != 0, paths[w * 32 : w * 32 + 32], 0.0)
            sums = sums + jnp.sum(t.reshape(4, 8, C), axis=0)
            row = t[:, 0:128]
            for q in range(1, C // 128):
                row = row + t[:, q * 128 : q * 128 + 128]
            at = slice(m * MC + w * 32, m * MC + w * 32 + 32)
            acc_r[at, :] = row if first else acc_r[at, :] + row
        return sums

    def send_cols(half, sums, first):
        whole = col_w * sums
        if first:
            whole = whole + col[0:1, :]
        for k in range(C // V):
            n = half * (C // V) + k
            cmsg[n, 0:1, 0:V] = whole[:, k * V : k * V + V]
            if first:
                cmsg[n, 1:2, 0:V] = col[1:2, k * V : k * V + V]
            else:
                cmsg[n, 1:2, 0:V] = jnp.zeros((1, V), F32)
        for k in range(C // V):
            n = half * (C // V) + k
            for g in range(2):
                @pl.when(jnp.logical_or(off, jnp.logical_or(n != c, g != h)))
                def _(n=n, g=g):
                    to_owner(n, g).start()

    kj(s, "p10")
    kj_words(b_own, s, 0, W)
    recv(m1.at[o], recv_sem.at[o])
    for n in range(8):
        go = bit_of(to_cols, n)

        @pl.when(go)
        def _(n=n, sent=sent):
            to_col(n, o, sent).start()

        sent = sent + go.astype(jnp.int32)

    @pl.when(diag)
    def _():
        hub_i[s] = hubw[...]

    def hub_half(half):
        pltpu.make_async_copy(hubw, hub_i.at[half], hub_recv.at[half]).wait()

    @pl.when(off)
    def _():
        hub_half(s)

    hub_half(o)
    G = hubw.shape[0]
    for half in range(2):
        for n, bits in enumerate(rows_of_bits(hub_i[half], 0, G)):
            r8[n * 32 : n * 32 + 32, half * C : half * C + C] = bits.astype(F32).astype(F8)
    reach = jnp.dot(r8[...], o8[...], preferred_element_type=F32)
    edge = hubw[...]
    lanes_c = jnp.concatenate([keep_cols_of(s, t) for t in range(C // 128)], axis=1)
    edge = edge & lanes_c
    hub_bits = jnp.concatenate(rows_of_bits(edge, 0, G), axis=0)
    meet = jnp.where(hub_bits != 0, reach, 0.0)
    hub_flag = hub_bits.astype(F32)

    def across(x):
        t = x[:, 0:128]
        for n in range(1, x.shape[1] // 128):
            t = t + x[:, n * 128 : n * 128 + 128]
        return jnp.sum(t.T, axis=0, keepdims=True)

    hub_tri = 0.5 * across(meet)
    hub_deg = across(hub_flag)
    hpart[...] = hub_tri

    def to_column(n):
        return pltpu.make_async_remote_copy(
            hpart, h_in.at[I], ha_send, ha_recv, device_id=(n, c, h), device_id_type=MESH
        )

    def others(act):
        for n in range(8):
            @pl.when(n != I)
            def _(n=n):
                act(n)

    others(lambda n: to_column(n).start())

    light_deg = jnp.sum(lax.population_count(mm1[s]).astype(F32), axis=0, keepdims=True) * 0.5
    edge_deg = jnp.sum(lax.population_count(edge).astype(F32), axis=0, keepdims=True)
    col[0:1, :] = jnp.sum(meet, axis=0, keepdims=True)
    col[1:2, :] = light_deg + jnp.where(diag, 1.0, 0.0) * edge_deg

    @pl.when(K != J)
    def _():
        recv(m2.at[0], recv_sem.at[2])

    @pl.when(K == J)
    def _():
        m2[...] = m1[...]

    @pl.when(K != J)
    def _():
        recv(m2.at[1], recv_sem.at[3])

    ik_rows(0)
    col_own = jnp.zeros((8, C), F32)
    for m in range(6):
        if m == 3:
            mask_half(o)
            kj(o, "p14")

        def beside(m=m):
            if m < 5:
                ik_rows(m + 1)
            if m >= 3:
                kj_words(b_other, o, (m - 3) * 16, 16)

        col_own = col_own + product(m, b_own, s, True, beside)
    sums = jnp.sum(col_own, axis=0, keepdims=True)
    col_other = jnp.zeros((8, C), F32)
    for m in range(6):
        col_other = col_other + product(m, b_other, o, False, lambda: None)
    pltpu.make_async_copy(h_in.at[pl.ds(0, 7)], h_in.at[pl.ds(0, 7)], ha_recv).wait()
    h_in[I] = hpart[...]
    send_cols(s, sums, True)
    send_cols(o, jnp.sum(col_other, axis=0, keepdims=True), False)

    hub_all = h_in[0]
    for n in range(1, 8):
        hub_all = hub_all + h_in[n]
    for n in range(B // V):
        rmsg[n, 0:1, 0:V] = jnp.sum(acc_r[n * V : n * V + V, :].T, axis=0, keepdims=True) * row_w
        rmsg[n, 1:2, :] = hub_all
        rmsg[n, 2:3, :] = hub_deg

    def to_plane(n):
        return pltpu.make_async_remote_copy(
            rmsg.at[n // 2],
            r_in.at[me],
            rs_sem,
            rr_sem,
            device_id=(I, n // 2, n % 2),
            device_id_type=MESH,
        )

    def plane(act):
        for n in range(32):
            @pl.when(n != me)
            def _(n=n):
                act(n)

    plane(lambda n: to_plane(n).start())
    r_in[me] = rmsg[c]

    @pl.when(diag)
    def _():
        c_in[I * 4 + s * 2 + h] = cmsg[c]

    vertex = I * B + c * V + lax.broadcasted_iota(jnp.int32, (V, 128), 0)
    is_hub = [vertex == ids_v[g : g + 1, :] for g in range(2)]
    each_hub(lambda d: d.wait_send())
    for n in range(MOST_SENDS):
        @pl.when(n < sent)
        def _(n=n):
            pltpu.make_async_copy(own, m2.at[s], send_sem.at[n]).wait()

    pltpu.make_async_copy(h_in.at[pl.ds(0, 7)], h_in.at[pl.ds(0, 7)], ha_send).wait()

    def wait_slots(ref, sem, count):
        part = ref.at[pl.ds(0, count)]
        pltpu.make_async_copy(part, part, sem).wait()

    def wait_cols(sem):
        @pl.when(off)
        def _():
            wait_slots(c_in, sem, 32)

        @pl.when(diag)
        def _():
            wait_slots(c_in, sem, 31)

    wait_cols(cr_sem)
    wait_slots(r_in, rr_sem, 31)
    even = r_in[0]
    odd = r_in[1]
    for n in range(1, 16):
        even = even + r_in[2 * n]
        odd = odd + r_in[2 * n + 1]
    both = even + odd
    cols = c_in[0]
    for n in range(1, 32):
        cols = cols + c_in[n]

    def at_hubs(r):
        rows = [jnp.broadcast_to(x[r : r + 1, :], (V, 128)) for x in (even, odd)]
        hit = jnp.where(is_hub[0], rows[0], 0.0) + jnp.where(is_hub[1], rows[1], 0.0)
        return jnp.sum(hit.T, axis=0, keepdims=True)

    tri = both[0:1, :V] + cols[0:1, :V] + at_hubs(1)
    deg = cols[1:2, :V] + at_hubs(2)
    out[...] = tri / (1.0 + deg)
    wait_cols(cs_sem)
    wait_slots(r_in, rs_sem, 31)


ROWS0_TO, ROWS1_TO, COLS_TO = destinations()
MOST_SENDS = 1 + max(
    sum(bin(x).count("1") for x in (r0, r1, *[c >> (8 * s) & 255 for s in (half, half)]))
    for r0, r1, c in zip(ROWS0_TO, ROWS1_TO, COLS_TO)
    for half in range(2)
)


def body(light_bits, hub_bits, hub_ids):
    W, C = light_bits.shape
    G = hub_bits.shape[0]
    B = 2 * C
    V = B // 16
    vmem = pl.BlockSpec(memory_space=pltpu.VMEM)
    out = pl.pallas_call(
        kernel,
        out_shape=jax.ShapeDtypeStruct((1, V), F32),
        in_specs=[pl.BlockSpec(memory_space=pltpu.HBM)] * 3,
        out_specs=vmem,
        scratch_shapes=[
            pltpu.SMEM((2, 128), jnp.int32),
            pltpu.VMEM((2, 128), jnp.int32),
            pltpu.VMEM((2, W, C), jnp.int32),
            pltpu.VMEM((2, W, C), jnp.int32),
            pltpu.VMEM((2, W, C), jnp.int32),
            pltpu.VMEM((2, W, C), jnp.int32),
            pltpu.VMEM((G, C), jnp.int32),
            pltpu.VMEM((2, G, C), jnp.int32),
            *[pltpu.VMEM((B // 6, B), F8)] * 6,
            pltpu.VMEM((B, C), F8),
            pltpu.VMEM((B, C), F8),
            pltpu.VMEM((B, C), F8),
            pltpu.VMEM((32 * G, B), F8),
            pltpu.VMEM((B, 128), F32),
            pltpu.VMEM((2, C), F32),
            pltpu.VMEM((1, 128), F32),
            pltpu.VMEM((8, 1, 128), F32),
            pltpu.VMEM((16, 4, 128), F32),
            pltpu.VMEM((16, 2, 128), F32),
            pltpu.VMEM((32, 4, 128), F32),
            pltpu.VMEM((32, 2, 128), F32),
            pltpu.SemaphoreType.DMA((4,)),
            pltpu.SemaphoreType.DMA((MOST_SENDS,)),
            pltpu.SemaphoreType.DMA((6,)),
            pltpu.SemaphoreType.DMA((16,)),
            pltpu.SemaphoreType.DMA((2,)),
            pltpu.SemaphoreType.DMA,
            pltpu.SemaphoreType.DMA,
            pltpu.SemaphoreType.DMA,
            pltpu.SemaphoreType.DMA,
            pltpu.SemaphoreType.DMA,
            pltpu.SemaphoreType.DMA,
        ],
        compiler_params=pltpu.CompilerParams(
            collective_id=0, has_side_effects=True, vmem_limit_bytes=67043328
        ),
    )(light_bits, hub_bits, hub_ids.reshape(2, 128))
    return out.reshape(V)


def solution(mesh):
    placed = (P("rows", "cols"), P("hub", "cols"), P())
    return jax.shard_map(body, mesh=mesh, in_specs=placed, out_specs=P(("rows", "cols")), check_vma=False)
```

```python
import functools

import jax
import jax.numpy as jnp
from jax import lax
from jax.experimental import pallas as pl
from jax.experimental.pallas import tpu as pltpu
from jax.sharding import PartitionSpec as P

MESH = pl.DeviceIdType.MESH
F32 = jnp.float32
F8 = jnp.float8_e4m3fn

THIRD = [
    0, 0, 47, 3, 42, 35, 59, 41, 28, 46, 60, 43, 52, 59, 46, 23,
    52, 17, 9, 9, 22, 4, 37, 26, 53, 34, 47, 20, 39, 22, 53, 59,
    62, 1, 11, 47, 18, 18, 17, 61, 4, 61, 33, 47, 48, 15, 37, 55,
    48, 20, 62, 1, 3, 38, 27, 27, 40, 52, 13, 52, 47, 52, 14, 56,
    15, 2, 25, 7, 11, 22, 11, 23, 36, 36, 25, 60, 62, 1, 59, 41,
    16, 49, 48, 11, 16, 51, 24, 58, 2, 46, 45, 45, 20, 48, 14, 7,
    13, 2, 13, 24, 35, 21, 1, 19, 42, 35, 43, 57, 54, 54, 46, 11,
    32, 25, 32, 17, 8, 26, 26, 44, 22, 4, 26, 44, 60, 16, 63, 63,
]


def nearer(j, k, h):
    here = j // 2 * 2 + h

    def hops(g):
        d = (k // 2 * 2 + g - here) % 8
        return min(d, 8 - d)

    return 1 - h if hops(1 - h) < hops(h) else h


def destinations():
    rows, cols = ([0] * 128, [0] * 128), [0] * 128
    for i in range(8):
        for j in range(8):
            for h in range(2):
                for s in range(2):
                    k = THIRD[(i * 8 + j) * 2 + h] >> (3 * s) & 7
                    if i != j and k != j:
                        rows[h][(i * 8 + k) * 2 + nearer(j, k, h)] |= 1 << (2 * j + s)
                    if i != j and k != i:
                        cols[((k * 8 + j) * 2 + h)] |= 1 << (8 * s + i)
    return rows[0], rows[1], cols


def lookup(tables, index, bits):
    tables = [list(t) for t in tables]
    for b in range(bits):
        odd = lax.rem(lax.div(index, 2**b), 2) == 1
        tables = [
            [x if isinstance(x, int) and x is y else jnp.where(odd, y, x) for x, y in zip(t[0::2], t[1::2])]
            for t in tables
        ]
    return [t[0] for t in tables]


def bit_of(mask, n):
    return lax.rem(lax.div(mask, 2**n), 2) == 1


def rows_of_bits(words, first, count):
    shift = lax.broadcasted_iota(jnp.int32, (32, words.shape[1]), 0)
    spread = [jnp.broadcast_to(words[w : w + 1, :], shift.shape) for w in range(first, first + count)]
    return [jnp.bitwise_and(jnp.right_shift(x, shift), 1) for x in spread]


def unpack_into(dst, src, words, lane=0):
    width = src.shape[1]

    def step(g, carry):
        block = src[pl.ds(pl.multiple_of(g * 8, 8), 8), :]
        for n, bits in enumerate(rows_of_bits(block, 0, 8)):
            at = pl.multiple_of(g * 256 + n * 32, 32)
            dst[pl.ds(at, 32), lane : lane + width] = bits.astype(F32).astype(dst.dtype)
        return carry

    lax.fori_loop(0, words // 8, step, 0)


def kernel(
    lb, hb, ids, out,
    ids_s, ids_v, m1, m2, m3, mm1, hubw, hub_i, a0, a1, a2, a3, a4, a5, b_own, b_other, o8, r8,
    acc_r, col, hpart, h_in, rmsg, cmsg, r_in, c_in,
    local_sem, send_sem, recv_sem, twin_sem, hub_send, hub_recv, ha_send, ha_recv, rs_sem, rr_sem, cs_sem, cr_sem,
):
    I = lax.axis_index("rows")
    c = lax.axis_index("cols")
    h = lax.axis_index("hub")
    J = lax.div(c, 2)
    s = lax.rem(c, 2)
    o = 1 - s
    W = m1.shape[1]
    C = m1.shape[2]
    B = 2 * C
    V = out.shape[1]
    diag = I == J
    off = jnp.logical_not(diag)
    me = c * 2 + h

    loads = [
        pltpu.make_async_copy(lb, m1.at[s], local_sem.at[0]),
        pltpu.make_async_copy(hb, hubw, local_sem.at[1]),
        pltpu.make_async_copy(ids, ids_s, local_sem.at[2]),
        pltpu.make_async_copy(ids, ids_v, local_sem.at[3]),
    ]
    for load in loads:
        load.start()

    barrier = pltpu.get_barrier_semaphore()

    def signal(dev):
        pl.semaphore_signal(barrier, inc=1, device_id=dev, device_id_type=MESH)

    signal((I, c + 1 - 2 * s, h))

    for n in range(1, 8):
        signal((lax.rem(I + n, 8), c, h))
    (thirds,) = lookup([THIRD], (I * 8 + J) * 2 + h, 7)
    K = lax.rem(jnp.where(s == 1, lax.div(thirds, 8), thirds), 8)
    ahead = lax.rem(lax.div(K, 2) - lax.div(J, 2) + 4, 4)
    near = jnp.where(ahead == 0, h, jnp.where(ahead == 1, 0, jnp.where(ahead == 3, 1, 1 - h)))

    @pl.when(jnp.logical_and(off, K != J))
    def _():
        for x in range(2):
            signal((I, 2 * K + x, near))

    @pl.when(jnp.logical_and(off, K != I))
    def _():
        signal((K, c, h))

    for x in range(2):
        for g in range(2):
            @pl.when(jnp.logical_or(off, jnp.logical_or(s != x, h != g)))
            def _(x=x, g=g):
                signal((I, 2 * I + x, g))

    to_rows0, to_rows1, to_cols = lookup([ROWS0_TO, ROWS1_TO, COLS_TO], (I * 8 + J) * 2 + h, 7)
    to_cols = lax.rem(jnp.where(s == 1, lax.div(to_cols, 256), to_cols), 256)
    readers = 0
    for mask, count in ((to_rows0, 16), (to_rows1, 16), (to_cols, 8)):
        for n in range(count):
            readers = readers + lax.rem(lax.div(mask, 2**n), 2)
    greeted = readers + jnp.where(diag, 39, 8)
    loads[0].wait()
    loads[1].wait()
    pl.semaphore_wait(barrier, greeted)

    own = m1.at[s]

    def to_row(n, g, sem):
        return pltpu.make_async_remote_copy(
            own, m2.at[s], send_sem.at[sem], recv_sem.at[2 + s], device_id=(I, n, g), device_id_type=MESH
        )

    def to_col(n, half, sem, rows=None):
        return pltpu.make_async_remote_copy(
            m1.at[half] if rows is None else m1.at[half, rows],
            m3.at[half] if rows is None else m3.at[half, rows],
            send_sem.at[sem],
            recv_sem.at[4 + half],
            device_id=(n, c, h),
            device_id_type=MESH,
        )

    pieces = [pl.ds(p * (W // 2), W // 2) for p in range(2)]

    def to_twin(p):
        return pltpu.make_async_remote_copy(
            m1.at[s, pieces[p]],
            m1.at[s, pieces[p]],
            send_sem.at[0],
            twin_sem.at[p],
            device_id=(I, c + 1 - 2 * s, h),
            device_id_type=MESH,
        )

    def to_hub(n):
        return pltpu.make_async_remote_copy(
            hubw, hub_i.at[s], hub_send.at[n], hub_recv.at[s], device_id=(I, n, h), device_id_type=MESH
        )

    def each_hub(act):
        @pl.when(diag)
        def _():
            for n in range(16):
                @pl.when(n != c)
                def _(n=n):
                    act(to_hub(n))

    each_hub(lambda d: d.start())
    to_twin(0).start()
    to_twin(1).start()
    sent = jnp.int32(1)
    for n in range(8):
        go = bit_of(to_cols, n)

        @pl.when(go)
        def _(n=n, sent=sent):
            to_col(n, s, sent).start()

        sent = sent + go.astype(jnp.int32)

    for g, mask in enumerate((to_rows0, to_rows1)):
        for n in range(16):
            go = bit_of(mask, n)

            @pl.when(go)
            def _(n=n, g=g, sent=sent):
                to_row(n, g, sent).start()

            sent = sent + go.astype(jnp.int32)

    loads[2].wait()
    loads[3].wait()
    lane_w = lax.broadcasted_iota(jnp.int32, (8, 128), 1)
    sub_w = lax.broadcasted_iota(jnp.int32, (8, 128), 0)
    word_id = jnp.where(sub_w == 0, I * W, K * W) + lane_w
    word_id = jnp.where(lane_w < W, word_id, -1)
    col_id = J * B + lax.broadcasted_iota(jnp.int32, (16, 128), 0) * 128 + lax.broadcasted_iota(jnp.int32, (16, 128), 1)

    def mark(g, carry):
        words, flags = carry
        for n in range(16):
            v = ids_s[lax.div(g, 8), lax.rem(g, 8) * 16 + n]
            words = words | jnp.where(
                word_id == jnp.right_shift(v, 5), jnp.left_shift(jnp.int32(1), jnp.bitwise_and(v, 31)), 0
            )
            flags = flags | (col_id == v).astype(jnp.int32)
        return words, flags

    words, flags = lax.fori_loop(
        0, 16, mark, (jnp.zeros((8, 128), jnp.int32), jnp.zeros((16, 128), jnp.int32))
    )
    keep_words = jnp.bitwise_not(words)
    keep_i = jnp.broadcast_to(keep_words[0:1, :], (128, 128)).T[:W]
    keep_k = jnp.broadcast_to(keep_words[1:2, :], (128, 128)).T[:W]
    keep_k_wide = jnp.concatenate([keep_k] * (C // 128), axis=1)
    keep_col = flags - 1

    def keep_cols_of(half, t):
        n = C // 128
        return jnp.where(half == 0, keep_col[t : t + 1, :], keep_col[n + t : n + t + 1, :])

    def mask_half(half):
        for t in range(C // 128):
            at = slice(t * 128, t * 128 + 128)
            mm1[half, :, at] = m1[half, :, at] & keep_i & keep_cols_of(half, t)

    mask_half(s)
    unpack_into(o8, mm1.at[s], W)

    def recv(ref, sem):
        pltpu.make_async_copy(own, ref, sem).wait()

    rows_ik = (a0, a1, a2, a3, a4, a5)
    row_w = jnp.where(diag, 0.125, jnp.where(K == I, 1.0, 0.5))
    col_w = jnp.where(diag, 0.0, jnp.where(K == J, 1.0, 0.5))
    MC = 256

    def to_owner(n, k):
        return pltpu.make_async_remote_copy(
            cmsg.at[n],
            c_in.at[I * 4 + s * 2 + h],
            cs_sem,
            cr_sem,
            device_id=(J, n, k),
            device_id_type=MESH,
        )

    def kj(half, name):
        @pl.when(K != I)
        def _():
            recv(m3.at[half], recv_sem.at[4 + half])

        @pl.when(K == I)
        def _():
            m3[half] = m1[half]


    def kj_words(dst, half, first, count):
        for g in range(first, first + count, 8):
            words = m3[half, g : g + 8, :] & keep_k_wide[g : g + 8, :]
            for n, bits in enumerate(rows_of_bits(words, 0, 8)):
                dst[(g + n) * 32 : (g + n) * 32 + 32, :] = bits.astype(F32).astype(F8)

    def ik_rows(m):
        for half in range(2):
            words = m2[half, m * 8 : m * 8 + 8, :]
            for n, bits in enumerate(rows_of_bits(words, 0, 8)):
                rows_ik[m][n * 32 : n * 32 + 32, half * C : half * C + C] = bits.astype(F32).astype(F8)

    def product(m, b8, half, first, beside):
        paths = jnp.dot(rows_ik[m][...], b8[...], preferred_element_type=F32)
        beside()
        words = mm1[half, m * 8 : m * 8 + 8, :]
        sums = jnp.zeros((8, C), F32)
        for w, bits in enumerate(rows_of_bits(words, 0, 8)):
            t = jnp.where(bits != 0, paths[w * 32 : w * 32 + 32], 0.0)
            sums = sums + jnp.sum(t.reshape(4, 8, C), axis=0)
            row = t[:, 0:128]
            for q in range(1, C // 128):
                row = row + t[:, q * 128 : q * 128 + 128]
            at = slice(m * MC + w * 32, m * MC + w * 32 + 32)
            acc_r[at, :] = row if first else acc_r[at, :] + row
        return sums

    def send_cols(half, sums, first):
        whole = col_w * sums
        if first:
            whole = whole + col[0:1, :]
        for k in range(C // V):
            n = half * (C // V) + k
            cmsg[n, 0:1, 0:V] = whole[:, k * V : k * V + V]
            if first:
                cmsg[n, 1:2, 0:V] = col[1:2, k * V : k * V + V]
            else:
                cmsg[n, 1:2, 0:V] = jnp.zeros((1, V), F32)
        for k in range(C // V):
            n = half * (C // V) + k
            for g in range(2):
                @pl.when(jnp.logical_or(off, jnp.logical_or(n != c, g != h)))
                def _(n=n, g=g):
                    to_owner(n, g).start()

    sent0 = sent
    for p in range(2):
        part = m1.at[o, pieces[p]]
        pltpu.make_async_copy(part, part, twin_sem.at[p]).wait()
        sent = sent0
        for n in range(8):
            go = bit_of(to_cols, n)

            @pl.when(go)
            def _(n=n, sent=sent, p=p):
                to_col(n, o, sent, pieces[p]).start()

            sent = sent + go.astype(jnp.int32)

    kj(s, "p10")
    kj_words(b_own, s, 0, W)
    @pl.when(diag)
    def _():
        hub_i[s] = hubw[...]

    def hub_half(half):
        pltpu.make_async_copy(hubw, hub_i.at[half], hub_recv.at[half]).wait()

    @pl.when(off)
    def _():
        hub_half(s)

    hub_half(o)
    G = hubw.shape[0]
    for half in range(2):
        for n, bits in enumerate(rows_of_bits(hub_i[half], 0, G)):
            r8[n * 32 : n * 32 + 32, half * C : half * C + C] = bits.astype(F32).astype(F8)
    reach = jnp.dot(r8[...], o8[...], preferred_element_type=F32)
    edge = hubw[...]
    lanes_c = jnp.concatenate([keep_cols_of(s, t) for t in range(C // 128)], axis=1)
    edge = edge & lanes_c
    hub_bits = jnp.concatenate(rows_of_bits(edge, 0, G), axis=0)
    meet = jnp.where(hub_bits != 0, reach, 0.0)
    hub_flag = hub_bits.astype(F32)

    def across(x):
        t = x[:, 0:128]
        for n in range(1, x.shape[1] // 128):
            t = t + x[:, n * 128 : n * 128 + 128]
        return jnp.sum(t.T, axis=0, keepdims=True)

    hub_tri = 0.5 * across(meet)
    hub_deg = across(hub_flag)
    hpart[...] = hub_tri

    def to_column(n):
        return pltpu.make_async_remote_copy(
            hpart, h_in.at[I], ha_send, ha_recv, device_id=(n, c, h), device_id_type=MESH
        )

    def others(act):
        for n in range(8):
            @pl.when(n != I)
            def _(n=n):
                act(n)

    others(lambda n: to_column(n).start())

    light_deg = jnp.sum(lax.population_count(mm1[s]).astype(F32), axis=0, keepdims=True) * 0.5
    edge_deg = jnp.sum(lax.population_count(edge).astype(F32), axis=0, keepdims=True)
    col[0:1, :] = jnp.sum(meet, axis=0, keepdims=True)
    col[1:2, :] = light_deg + jnp.where(diag, 1.0, 0.0) * edge_deg

    @pl.when(K != J)
    def _():
        recv(m2.at[0], recv_sem.at[2])

    @pl.when(K == J)
    def _():
        m2[...] = m1[...]

    @pl.when(K != J)
    def _():
        recv(m2.at[1], recv_sem.at[3])

    ik_rows(0)
    col_own = jnp.zeros((8, C), F32)
    for m in range(6):
        if m == 3:
            mask_half(o)
            kj(o, "p14")

        def beside(m=m):
            if m < 5:
                ik_rows(m + 1)
            if m >= 3:
                kj_words(b_other, o, (m - 3) * 16, 16)

        col_own = col_own + product(m, b_own, s, True, beside)
    sums = jnp.sum(col_own, axis=0, keepdims=True)
    col_other = jnp.zeros((8, C), F32)

    def row_sums(first, last):
        for n in range(B // V):
            if first * MC < n * V + V <= last * MC:
                rmsg[n, 0:1, 0:V] = jnp.sum(acc_r[n * V : n * V + V, :].T, axis=0, keepdims=True) * row_w

    for m in range(6):
        col_other = col_other + product(m, b_other, o, False, lambda m=m: row_sums(m - 1, m))
    pltpu.make_async_copy(h_in.at[pl.ds(0, 7)], h_in.at[pl.ds(0, 7)], ha_recv).wait()
    h_in[I] = hpart[...]
    send_cols(s, sums, True)
    send_cols(o, jnp.sum(col_other, axis=0, keepdims=True), False)

    row_sums(5, 6)
    hub_all = h_in[0]
    for n in range(1, 8):
        hub_all = hub_all + h_in[n]
    for n in range(B // V):
        rmsg[n, 1:2, :] = hub_all
        rmsg[n, 2:3, :] = hub_deg

    def to_plane(n):
        return pltpu.make_async_remote_copy(
            rmsg.at[n // 2],
            r_in.at[me],
            rs_sem,
            rr_sem,
            device_id=(I, n // 2, n % 2),
            device_id_type=MESH,
        )

    def plane(act):
        for n in range(32):
            @pl.when(n != me)
            def _(n=n):
                act(n)

    plane(lambda n: to_plane(n).start())
    r_in[me] = rmsg[c]

    @pl.when(diag)
    def _():
        c_in[I * 4 + s * 2 + h] = cmsg[c]

    vertex = I * B + c * V + lax.broadcasted_iota(jnp.int32, (V, 128), 0)
    is_hub = [vertex == ids_v[g : g + 1, :] for g in range(2)]
    each_hub(lambda d: d.wait_send())
    for n in range(MOST_SENDS):
        @pl.when(n < sent)
        def _(n=n):
            pltpu.make_async_copy(own, m2.at[s], send_sem.at[n]).wait()

    pltpu.make_async_copy(h_in.at[pl.ds(0, 7)], h_in.at[pl.ds(0, 7)], ha_send).wait()

    def wait_slots(ref, sem, count):
        part = ref.at[pl.ds(0, count)]
        pltpu.make_async_copy(part, part, sem).wait()

    def wait_cols(sem):
        @pl.when(off)
        def _():
            wait_slots(c_in, sem, 32)

        @pl.when(diag)
        def _():
            wait_slots(c_in, sem, 31)

    wait_cols(cr_sem)
    wait_slots(r_in, rr_sem, 31)
    even = r_in[0]
    odd = r_in[1]
    for n in range(1, 16):
        even = even + r_in[2 * n]
        odd = odd + r_in[2 * n + 1]
    both = even + odd
    cols = c_in[0]
    for n in range(1, 32):
        cols = cols + c_in[n]

    def at_hubs(r):
        rows = [jnp.broadcast_to(x[r : r + 1, :], (V, 128)) for x in (even, odd)]
        hit = jnp.where(is_hub[0], rows[0], 0.0) + jnp.where(is_hub[1], rows[1], 0.0)
        return jnp.sum(hit.T, axis=0, keepdims=True)

    tri = both[0:1, :V] + cols[0:1, :V] + at_hubs(1)
    deg = cols[1:2, :V] + at_hubs(2)
    out[...] = tri / (1.0 + deg)
    wait_cols(cs_sem)
    wait_slots(r_in, rs_sem, 31)


ROWS0_TO, ROWS1_TO, COLS_TO = destinations()
MOST_SENDS = 1 + max(
    sum(bin(x).count("1") for x in (r0, r1, *[c >> (8 * s) & 255 for s in (half, half)]))
    for r0, r1, c in zip(ROWS0_TO, ROWS1_TO, COLS_TO)
    for half in range(2)
)


def body(light_bits, hub_bits, hub_ids):
    W, C = light_bits.shape
    G = hub_bits.shape[0]
    B = 2 * C
    V = B // 16
    vmem = pl.BlockSpec(memory_space=pltpu.VMEM)
    out = pl.pallas_call(
        kernel,
        out_shape=jax.ShapeDtypeStruct((1, V), F32),
        in_specs=[pl.BlockSpec(memory_space=pltpu.HBM)] * 3,
        out_specs=vmem,
        scratch_shapes=[
            pltpu.SMEM((2, 128), jnp.int32),
            pltpu.VMEM((2, 128), jnp.int32),
            pltpu.VMEM((2, W, C), jnp.int32),
            pltpu.VMEM((2, W, C), jnp.int32),
            pltpu.VMEM((2, W, C), jnp.int32),
            pltpu.VMEM((2, W, C), jnp.int32),
            pltpu.VMEM((G, C), jnp.int32),
            pltpu.VMEM((2, G, C), jnp.int32),
            *[pltpu.VMEM((B // 6, B), F8)] * 6,
            pltpu.VMEM((B, C), F8),
            pltpu.VMEM((B, C), F8),
            pltpu.VMEM((B, C), F8),
            pltpu.VMEM((32 * G, B), F8),
            pltpu.VMEM((B, 128), F32),
            pltpu.VMEM((2, C), F32),
            pltpu.VMEM((1, 128), F32),
            pltpu.VMEM((8, 1, 128), F32),
            pltpu.VMEM((16, 4, 128), F32),
            pltpu.VMEM((16, 2, 128), F32),
            pltpu.VMEM((32, 4, 128), F32),
            pltpu.VMEM((32, 2, 128), F32),
            pltpu.SemaphoreType.DMA((4,)),
            pltpu.SemaphoreType.DMA((MOST_SENDS,)),
            pltpu.SemaphoreType.DMA((6,)),
            pltpu.SemaphoreType.DMA((2,)),
            pltpu.SemaphoreType.DMA((16,)),
            pltpu.SemaphoreType.DMA((2,)),
            pltpu.SemaphoreType.DMA,
            pltpu.SemaphoreType.DMA,
            pltpu.SemaphoreType.DMA,
            pltpu.SemaphoreType.DMA,
            pltpu.SemaphoreType.DMA,
            pltpu.SemaphoreType.DMA,
        ],
        compiler_params=pltpu.CompilerParams(
            collective_id=0, has_side_effects=True, vmem_limit_bytes=56550000
        ),
    )(light_bits, hub_bits, hub_ids.reshape(2, 128))
    return out.reshape(V)


def solution(mesh):
    placed = (P("rows", "cols"), P("hub", "cols"), P())
    return jax.shard_map(body, mesh=mesh, in_specs=placed, out_specs=P(("rows", "cols")), check_vma=False)
```

```python
import functools

import jax
import jax.numpy as jnp
from jax import lax
from jax.experimental import pallas as pl
from jax.experimental.pallas import tpu as pltpu
from jax.sharding import PartitionSpec as P

MESH = pl.DeviceIdType.MESH
F32 = jnp.float32
F8 = jnp.float8_e4m3fn

THIRD = [
    0, 0, 57, 29, 42, 35, 47, 25, 55, 44, 11, 61, 44, 62, 15, 43,
    48, 20, 9, 9, 6, 20, 19, 44, 32, 22, 46, 23, 6, 34, 37, 55,
    14, 56, 57, 29, 18, 18, 25, 47, 37, 55, 41, 59, 53, 60, 57, 29,
    48, 34, 7, 49, 16, 52, 27, 27, 6, 34, 12, 46, 32, 22, 44, 55,
    17, 24, 43, 15, 24, 10, 13, 59, 36, 36, 25, 47, 30, 7, 43, 57,
    4, 50, 24, 33, 2, 38, 19, 7, 16, 52, 45, 45, 50, 32, 7, 14,
    1, 19, 29, 57, 17, 24, 41, 59, 10, 37, 29, 15, 54, 54, 29, 57,
    34, 6, 8, 19, 4, 50, 10, 24, 20, 6, 35, 42, 34, 48, 63, 63,
]


def nearer(j, k, h):
    here = j // 2 * 2 + h

    def hops(g):
        d = (k // 2 * 2 + g - here) % 8
        return min(d, 8 - d)

    return 1 - h if hops(1 - h) < hops(h) else h


def destinations():
    rows, cols = ([0] * 128, [0] * 128), [0] * 128
    for i in range(8):
        for j in range(8):
            for h in range(2):
                for s in range(2):
                    k = THIRD[(i * 8 + j) * 2 + h] >> (3 * s) & 7
                    if i != j and k != j:
                        rows[h][(i * 8 + k) * 2 + nearer(j, k, h)] |= 1 << (2 * j + s)
                    if i != j and k != i:
                        cols[((k * 8 + j) * 2 + h)] |= 1 << (8 * s + i)
    return rows[0], rows[1], cols


def lookup(tables, index, bits):
    tables = [list(t) for t in tables]
    for b in range(bits):
        odd = lax.rem(lax.div(index, 2**b), 2) == 1
        tables = [
            [x if isinstance(x, int) and x is y else jnp.where(odd, y, x) for x, y in zip(t[0::2], t[1::2])]
            for t in tables
        ]
    return [t[0] for t in tables]


def bit_of(mask, n):
    return lax.rem(lax.div(mask, 2**n), 2) == 1


def rows_of_bits(words, first, count):
    shift = lax.broadcasted_iota(jnp.int32, (32, words.shape[1]), 0)
    spread = [jnp.broadcast_to(words[w : w + 1, :], shift.shape) for w in range(first, first + count)]
    return [jnp.bitwise_and(jnp.right_shift(x, shift), 1) for x in spread]


def unpack_into(dst, src, words, lane=0):
    width = src.shape[1]

    def step(g, carry):
        block = src[pl.ds(pl.multiple_of(g * 8, 8), 8), :]
        for n, bits in enumerate(rows_of_bits(block, 0, 8)):
            at = pl.multiple_of(g * 256 + n * 32, 32)
            dst[pl.ds(at, 32), lane : lane + width] = bits.astype(F32).astype(dst.dtype)
        return carry

    lax.fori_loop(0, words // 8, step, 0)


def kernel(
    lb, hb, ids, out,
    ids_s, ids_v, m1, m2, m3, mm1, hubw, hub_i, a0, a1, a2, a3, a4, a5, b_own, b_other, o8, r8,
    acc_r, col, hpart, h_in, rmsg, cmsg, r_in, c_in,
    local_sem, send_sem, recv_sem, twin_sem, row_sem, hub_send, hub_recv, ha_send, ha_recv, rs_sem, rr_sem, cs_sem, cr_sem,
):
    I = lax.axis_index("rows")
    c = lax.axis_index("cols")
    h = lax.axis_index("hub")
    J = lax.div(c, 2)
    s = lax.rem(c, 2)
    o = 1 - s
    W = m1.shape[1]
    C = m1.shape[2]
    B = 2 * C
    V = out.shape[1]
    diag = I == J
    off = jnp.logical_not(diag)
    me = c * 2 + h

    loads = [
        pltpu.make_async_copy(lb, m1.at[s], local_sem.at[0]),
        pltpu.make_async_copy(hb, hubw, local_sem.at[1]),
        pltpu.make_async_copy(ids, ids_s, local_sem.at[2]),
        pltpu.make_async_copy(ids, ids_v, local_sem.at[3]),
    ]
    for load in loads:
        load.start()

    barrier = pltpu.get_barrier_semaphore()

    def signal(dev):
        pl.semaphore_signal(barrier, inc=1, device_id=dev, device_id_type=MESH)

    signal((I, c + 1 - 2 * s, h))

    for n in range(1, 8):
        signal((lax.rem(I + n, 8), c, h))
    (thirds,) = lookup([THIRD], (I * 8 + J) * 2 + h, 7)
    K = lax.rem(jnp.where(s == 1, lax.div(thirds, 8), thirds), 8)
    ahead = lax.rem(lax.div(K, 2) - lax.div(J, 2) + 4, 4)
    near = jnp.where(ahead == 0, h, jnp.where(ahead == 1, 0, jnp.where(ahead == 3, 1, 1 - h)))

    @pl.when(jnp.logical_and(off, K != J))
    def _():
        for x in range(2):
            signal((I, 2 * K + x, near))

    @pl.when(jnp.logical_and(off, K != I))
    def _():
        signal((K, c, h))

    for x in range(2):
        for g in range(2):
            @pl.when(jnp.logical_or(off, jnp.logical_or(s != x, h != g)))
            def _(x=x, g=g):
                signal((I, 2 * I + x, g))

    to_rows0, to_rows1, to_cols = lookup([ROWS0_TO, ROWS1_TO, COLS_TO], (I * 8 + J) * 2 + h, 7)
    to_cols = lax.rem(jnp.where(s == 1, lax.div(to_cols, 256), to_cols), 256)
    readers = 0
    for mask, count in ((to_rows0, 16), (to_rows1, 16), (to_cols, 8)):
        for n in range(count):
            readers = readers + lax.rem(lax.div(mask, 2**n), 2)
    greeted = readers + jnp.where(diag, 39, 8)
    loads[0].wait()
    loads[1].wait()
    pl.semaphore_wait(barrier, greeted)

    own = m1.at[s]

    ik_pieces = [pl.ds(0, 2 * W // 3), pl.ds(2 * W // 3, W // 3)]

    def to_row(n, g, sem, p):
        return pltpu.make_async_remote_copy(
            m1.at[s, ik_pieces[p]],
            m2.at[s, ik_pieces[p]],
            send_sem.at[sem],
            row_sem.at[2 * p + s],
            device_id=(I, n, g),
            device_id_type=MESH,
        )

    def to_col(n, half, sem, rows=None):
        return pltpu.make_async_remote_copy(
            m1.at[half] if rows is None else m1.at[half, rows],
            m3.at[half] if rows is None else m3.at[half, rows],
            send_sem.at[sem],
            recv_sem.at[4 + half],
            device_id=(n, c, h),
            device_id_type=MESH,
        )

    pieces = [pl.ds(p * (W // 2), W // 2) for p in range(2)]

    def to_twin(p):
        return pltpu.make_async_remote_copy(
            m1.at[s, pieces[p]],
            m1.at[s, pieces[p]],
            send_sem.at[0],
            twin_sem.at[p],
            device_id=(I, c + 1 - 2 * s, h),
            device_id_type=MESH,
        )

    def to_hub(n):
        return pltpu.make_async_remote_copy(
            hubw, hub_i.at[s], hub_send.at[n], hub_recv.at[s], device_id=(I, n, h), device_id_type=MESH
        )

    def each_hub(act):
        @pl.when(diag)
        def _():
            for n in range(16):
                @pl.when(n != c)
                def _(n=n):
                    act(to_hub(n))

    each_hub(lambda d: d.start())
    to_twin(0).start()
    to_twin(1).start()
    sent = jnp.int32(1)
    for n in range(8):
        go = bit_of(to_cols, n)

        @pl.when(go)
        def _(n=n, sent=sent):
            to_col(n, s, sent).start()

        sent = sent + go.astype(jnp.int32)

    def send_rows(p, sent):
        for g, mask in enumerate((to_rows0, to_rows1)):
            for n in range(16):
                go = bit_of(mask, n)

                @pl.when(go)
                def _(n=n, g=g, sent=sent):
                    to_row(n, g, sent, p).start()

                sent = sent + go.astype(jnp.int32)
        return sent

    first_row = sent
    sent = send_rows(0, first_row)

    loads[2].wait()
    loads[3].wait()
    lane_w = lax.broadcasted_iota(jnp.int32, (8, 128), 1)
    sub_w = lax.broadcasted_iota(jnp.int32, (8, 128), 0)
    word_id = jnp.where(sub_w == 0, I * W, K * W) + lane_w
    word_id = jnp.where(lane_w < W, word_id, -1)
    col_id = J * B + lax.broadcasted_iota(jnp.int32, (16, 128), 0) * 128 + lax.broadcasted_iota(jnp.int32, (16, 128), 1)

    def mark(g, carry):
        words, flags = carry
        for n in range(16):
            v = ids_s[lax.div(g, 8), lax.rem(g, 8) * 16 + n]
            words = words | jnp.where(
                word_id == jnp.right_shift(v, 5), jnp.left_shift(jnp.int32(1), jnp.bitwise_and(v, 31)), 0
            )
            flags = flags | (col_id == v).astype(jnp.int32)
        return words, flags

    words, flags = lax.fori_loop(
        0, 16, mark, (jnp.zeros((8, 128), jnp.int32), jnp.zeros((16, 128), jnp.int32))
    )
    keep_words = jnp.bitwise_not(words)
    keep_i = jnp.broadcast_to(keep_words[0:1, :], (128, 128)).T[:W]
    keep_k = jnp.broadcast_to(keep_words[1:2, :], (128, 128)).T[:W]
    keep_k_wide = jnp.concatenate([keep_k] * (C // 128), axis=1)
    keep_col = flags - 1

    def keep_cols_of(half, t):
        n = C // 128
        return jnp.where(half == 0, keep_col[t : t + 1, :], keep_col[n + t : n + t + 1, :])

    def mask_half(half):
        for t in range(C // 128):
            at = slice(t * 128, t * 128 + 128)
            mm1[half, :, at] = m1[half, :, at] & keep_i & keep_cols_of(half, t)

    mask_half(s)
    unpack_into(o8, mm1.at[s], W)

    def recv(ref, sem):
        pltpu.make_async_copy(own, ref, sem).wait()

    rows_ik = (a0, a1, a2, a3, a4, a5)
    row_w = jnp.where(diag, 0.125, jnp.where(K == I, 1.0, 0.5))
    col_w = jnp.where(diag, 0.0, jnp.where(K == J, 1.0, 0.5))
    MC = 256

    def to_owner(n, k):
        return pltpu.make_async_remote_copy(
            cmsg.at[n],
            c_in.at[I * 4 + s * 2 + h],
            cs_sem,
            cr_sem,
            device_id=(J, n, k),
            device_id_type=MESH,
        )

    def kj(half, name):
        @pl.when(K != I)
        def _():
            recv(m3.at[half], recv_sem.at[4 + half])

        @pl.when(K == I)
        def _():
            m3[half] = m1[half]


    def kj_words(dst, half, first, count):
        for g in range(first, first + count, 8):
            words = m3[half, g : g + 8, :] & keep_k_wide[g : g + 8, :]
            for n, bits in enumerate(rows_of_bits(words, 0, 8)):
                dst[(g + n) * 32 : (g + n) * 32 + 32, :] = bits.astype(F32).astype(F8)

    def ik_rows(m):
        for half in range(2):
            words = m2[half, m * 8 : m * 8 + 8, :]
            for n, bits in enumerate(rows_of_bits(words, 0, 8)):
                rows_ik[m][n * 32 : n * 32 + 32, half * C : half * C + C] = bits.astype(F32).astype(F8)

    def product(m, b8, half, first, beside):
        paths = jnp.dot(rows_ik[m][...], b8[...], preferred_element_type=F32)
        beside()
        words = mm1[half, m * 8 : m * 8 + 8, :]
        sums = jnp.zeros((8, C), F32)
        for w, bits in enumerate(rows_of_bits(words, 0, 8)):
            t = jnp.where(bits != 0, paths[w * 32 : w * 32 + 32], 0.0)
            sums = sums + jnp.sum(t.reshape(4, 8, C), axis=0)
            row = t[:, 0:128]
            for q in range(1, C // 128):
                row = row + t[:, q * 128 : q * 128 + 128]
            at = slice(m * MC + w * 32, m * MC + w * 32 + 32)
            acc_r[at, :] = row if first else acc_r[at, :] + row
        return sums

    def send_cols(half, sums, first):
        whole = col_w * sums
        if first:
            whole = whole + col[0:1, :]
        for k in range(C // V):
            n = half * (C // V) + k
            cmsg[n, 0:1, 0:V] = whole[:, k * V : k * V + V]
            if first:
                cmsg[n, 1:2, 0:V] = col[1:2, k * V : k * V + V]
            else:
                cmsg[n, 1:2, 0:V] = jnp.zeros((1, V), F32)
        for k in range(C // V):
            n = half * (C // V) + k
            for g in range(2):
                @pl.when(jnp.logical_or(off, jnp.logical_or(n != c, g != h)))
                def _(n=n, g=g):
                    to_owner(n, g).start()

    first_relay = sent

    def relay(p):
        part = m1.at[o, pieces[p]]
        pltpu.make_async_copy(part, part, twin_sem.at[p]).wait()
        sent = first_relay
        for n in range(8):
            go = bit_of(to_cols, n)

            @pl.when(go)
            def _(n=n, sent=sent):
                to_col(n, o, sent, pieces[p]).start()

            sent = sent + go.astype(jnp.int32)
        return sent

    relay(0)
    send_rows(1, first_row)
    kj(s, "p10")
    kj_words(b_own, s, 0, W)
    sent = relay(1)
    @pl.when(diag)
    def _():
        hub_i[s] = hubw[...]

    def hub_half(half):
        pltpu.make_async_copy(hubw, hub_i.at[half], hub_recv.at[half]).wait()

    @pl.when(off)
    def _():
        hub_half(s)

    hub_half(o)
    G = hubw.shape[0]
    for half in range(2):
        for n, bits in enumerate(rows_of_bits(hub_i[half], 0, G)):
            r8[n * 32 : n * 32 + 32, half * C : half * C + C] = bits.astype(F32).astype(F8)
    reach = jnp.dot(r8[...], o8[...], preferred_element_type=F32)
    edge = hubw[...]
    lanes_c = jnp.concatenate([keep_cols_of(s, t) for t in range(C // 128)], axis=1)
    edge = edge & lanes_c
    hub_bits = jnp.concatenate(rows_of_bits(edge, 0, G), axis=0)
    meet = jnp.where(hub_bits != 0, reach, 0.0)
    hub_flag = hub_bits.astype(F32)

    def across(x):
        t = x[:, 0:128]
        for n in range(1, x.shape[1] // 128):
            t = t + x[:, n * 128 : n * 128 + 128]
        return jnp.sum(t.T, axis=0, keepdims=True)

    hub_tri = 0.5 * across(meet)
    hub_deg = across(hub_flag)
    hpart[...] = hub_tri

    def to_column(n):
        return pltpu.make_async_remote_copy(
            hpart, h_in.at[I], ha_send, ha_recv, device_id=(n, c, h), device_id_type=MESH
        )

    def others(act):
        for n in range(8):
            @pl.when(n != I)
            def _(n=n):
                act(n)

    others(lambda n: to_column(n).start())

    light_deg = jnp.sum(lax.population_count(mm1[s]).astype(F32), axis=0, keepdims=True) * 0.5
    edge_deg = jnp.sum(lax.population_count(edge).astype(F32), axis=0, keepdims=True)
    col[0:1, :] = jnp.sum(meet, axis=0, keepdims=True)
    col[1:2, :] = light_deg + jnp.where(diag, 1.0, 0.0) * edge_deg


    def ik_wait(p):
        for half in range(2):
            part = m2.at[half, ik_pieces[p]]
            pltpu.make_async_copy(part, part, row_sem.at[2 * p + half]).wait()

    @pl.when(K != J)
    def _():
        ik_wait(0)

    @pl.when(K == J)
    def _():
        m2[...] = m1[...]

    ik_rows(0)
    col_own = jnp.zeros((8, C), F32)
    for m in range(6):
        if m == 3:
            @pl.when(K != J)
            def _():
                ik_wait(1)

            mask_half(o)
            kj(o, "p14")

        def beside(m=m):
            if m < 5:
                ik_rows(m + 1)
            if m >= 3:
                kj_words(b_other, o, (m - 3) * 16, 16)

        col_own = col_own + product(m, b_own, s, True, beside)
    sums = jnp.sum(col_own, axis=0, keepdims=True)
    col_other = jnp.zeros((8, C), F32)

    def row_sums(first, last):
        for n in range(B // V):
            if first * MC < n * V + V <= last * MC:
                rmsg[n, 0:1, 0:V] = jnp.sum(acc_r[n * V : n * V + V, :].T, axis=0, keepdims=True) * row_w

    for m in range(6):
        col_other = col_other + product(m, b_other, o, False, lambda m=m: row_sums(m - 1, m))
    pltpu.make_async_copy(h_in.at[pl.ds(0, 7)], h_in.at[pl.ds(0, 7)], ha_recv).wait()
    h_in[I] = hpart[...]
    send_cols(s, sums, True)
    send_cols(o, jnp.sum(col_other, axis=0, keepdims=True), False)

    row_sums(5, 6)
    hub_all = h_in[0]
    for n in range(1, 8):
        hub_all = hub_all + h_in[n]
    for n in range(B // V):
        rmsg[n, 1:2, :] = hub_all
        rmsg[n, 2:3, :] = hub_deg

    def to_plane(n):
        return pltpu.make_async_remote_copy(
            rmsg.at[n // 2],
            r_in.at[me],
            rs_sem,
            rr_sem,
            device_id=(I, n // 2, n % 2),
            device_id_type=MESH,
        )

    def plane(act):
        for n in range(32):
            @pl.when(n != me)
            def _(n=n):
                act(n)

    plane(lambda n: to_plane(n).start())
    r_in[me] = rmsg[c]

    @pl.when(diag)
    def _():
        c_in[I * 4 + s * 2 + h] = cmsg[c]

    vertex = I * B + c * V + lax.broadcasted_iota(jnp.int32, (V, 128), 0)
    is_hub = [vertex == ids_v[g : g + 1, :] for g in range(2)]
    each_hub(lambda d: d.wait_send())
    for n in range(MOST_SENDS):
        @pl.when(n < sent)
        def _(n=n):
            pltpu.make_async_copy(own, m2.at[s], send_sem.at[n]).wait()

    pltpu.make_async_copy(h_in.at[pl.ds(0, 7)], h_in.at[pl.ds(0, 7)], ha_send).wait()

    def wait_slots(ref, sem, count):
        part = ref.at[pl.ds(0, count)]
        pltpu.make_async_copy(part, part, sem).wait()

    def wait_cols(sem):
        @pl.when(off)
        def _():
            wait_slots(c_in, sem, 32)

        @pl.when(diag)
        def _():
            wait_slots(c_in, sem, 31)

    wait_cols(cr_sem)
    wait_slots(r_in, rr_sem, 31)
    even = r_in[0]
    odd = r_in[1]
    for n in range(1, 16):
        even = even + r_in[2 * n]
        odd = odd + r_in[2 * n + 1]
    both = even + odd
    cols = c_in[0]
    for n in range(1, 32):
        cols = cols + c_in[n]

    def at_hubs(r):
        rows = [jnp.broadcast_to(x[r : r + 1, :], (V, 128)) for x in (even, odd)]
        hit = jnp.where(is_hub[0], rows[0], 0.0) + jnp.where(is_hub[1], rows[1], 0.0)
        return jnp.sum(hit.T, axis=0, keepdims=True)

    tri = both[0:1, :V] + cols[0:1, :V] + at_hubs(1)
    deg = cols[1:2, :V] + at_hubs(2)
    out[...] = tri / (1.0 + deg)
    wait_cols(cs_sem)
    wait_slots(r_in, rs_sem, 31)


ROWS0_TO, ROWS1_TO, COLS_TO = destinations()
MOST_SENDS = 1 + max(
    sum(bin(x).count("1") for x in (r0, r1, *[c >> (8 * s) & 255 for s in (half, half)]))
    for r0, r1, c in zip(ROWS0_TO, ROWS1_TO, COLS_TO)
    for half in range(2)
)


def body(light_bits, hub_bits, hub_ids):
    W, C = light_bits.shape
    G = hub_bits.shape[0]
    B = 2 * C
    V = B // 16
    vmem = pl.BlockSpec(memory_space=pltpu.VMEM)
    out = pl.pallas_call(
        kernel,
        out_shape=jax.ShapeDtypeStruct((1, V), F32),
        in_specs=[pl.BlockSpec(memory_space=pltpu.HBM)] * 3,
        out_specs=vmem,
        scratch_shapes=[
            pltpu.SMEM((2, 128), jnp.int32),
            pltpu.VMEM((2, 128), jnp.int32),
            pltpu.VMEM((2, W, C), jnp.int32),
            pltpu.VMEM((2, W, C), jnp.int32),
            pltpu.VMEM((2, W, C), jnp.int32),
            pltpu.VMEM((2, W, C), jnp.int32),
            pltpu.VMEM((G, C), jnp.int32),
            pltpu.VMEM((2, G, C), jnp.int32),
            *[pltpu.VMEM((B // 6, B), F8)] * 6,
            pltpu.VMEM((B, C), F8),
            pltpu.VMEM((B, C), F8),
            pltpu.VMEM((B, C), F8),
            pltpu.VMEM((32 * G, B), F8),
            pltpu.VMEM((B, 128), F32),
            pltpu.VMEM((2, C), F32),
            pltpu.VMEM((1, 128), F32),
            pltpu.VMEM((8, 1, 128), F32),
            pltpu.VMEM((16, 4, 128), F32),
            pltpu.VMEM((16, 2, 128), F32),
            pltpu.VMEM((32, 4, 128), F32),
            pltpu.VMEM((32, 2, 128), F32),
            pltpu.SemaphoreType.DMA((4,)),
            pltpu.SemaphoreType.DMA((MOST_SENDS,)),
            pltpu.SemaphoreType.DMA((6,)),
            pltpu.SemaphoreType.DMA((2,)),
            pltpu.SemaphoreType.DMA((4,)),
            pltpu.SemaphoreType.DMA((16,)),
            pltpu.SemaphoreType.DMA((2,)),
            pltpu.SemaphoreType.DMA,
            pltpu.SemaphoreType.DMA,
            pltpu.SemaphoreType.DMA,
            pltpu.SemaphoreType.DMA,
            pltpu.SemaphoreType.DMA,
            pltpu.SemaphoreType.DMA,
        ],
        compiler_params=pltpu.CompilerParams(
            collective_id=0, has_side_effects=True, vmem_limit_bytes=56550000
        ),
    )(light_bits, hub_bits, hub_ids.reshape(2, 128))
    return out.reshape(V)


def solution(mesh):
    placed = (P("rows", "cols"), P("hub", "cols"), P())
    return jax.shard_map(body, mesh=mesh, in_specs=placed, out_specs=P(("rows", "cols")), check_vma=False)
```
